128 devices in a mesh: rows: 16 (over z, x), grid: 8 (over y, core).
Axes of the slice: x: 4, y: 4, z: 4, core: 2. Of those that a mesh axis runs over, the one named last changes fastest.
Arguments:
- design: bfloat16 [393216, 1024], P(('rows', 'grid')), may hold values from -24 to 24
- observed: float32 [393216], P(('rows', 'grid')), may hold values from -6 to 6
- weight_class: int32 [393216], P(('rows', 'grid')), may hold values from 0 to 15
- calib_unit: int32 [393216], P(('rows', 'grid')), may hold values from 0 to 63
- class_weight: float32 [16], replicated, may hold values from 0.5 to 8
- calib_scale: float32 [64, 8], replicated, may hold values from 0.5 to 2
Outputs:
- normal_matrix: float32 [1024, 1024], P('rows', 'grid')
- right_hand: float32 [1024], P(('rows', 'grid'))
- chi_square: float32 [], replicated
The draws below stay inside these ranges and needn't reach their ends.
All inputs are finite; a program needn't handle non-finite values.
Results may differ from the reference program's by a relative error of at most 0.01.
Values sent between devices are 32-bit elements; how exact they have to be, the bound alone decides.
A program may use at most 64 MiB of HBM per device.

```python
import math
import jax
import jax.numpy as jnp
from jax import lax

P_SIZE = 1024
CB = 128
NB = 8
UNITS = 64
CLASSES = 16
ROW_DEV = 3072
NROWS = 393216


def set_ends(result, own_key, low, high):
    index_at = [jax.random.randint(jax.random.fold_in(own_key, axis), (), 0, length) for axis, length in enumerate(result.shape)]
    longest = result.shape.index(max(result.shape))
    neighbour = index_at[:longest] + [(index_at[longest] + 1) % result.shape[longest]] + index_at[longest + 1:]
    return result.at[tuple(index_at)].set(low).at[tuple(neighbour)].set(high)


def strengthened(array, rng, source, target, blocks, factor):
    owner, partner = [(jnp.arange(array.shape[dim]) // (array.shape[dim] // blocks)).reshape([-1 if axis == dim else 1 for axis in range(array.ndim)]) for dim in (source, target)]
    chosen = jax.random.permutation(rng, blocks)[partner]
    strong = (owner == chosen) | (owner == (partner + blocks // 2) % blocks)
    return jnp.where(strong, factor * array, array)


def block_scale(key, shape, pieces, least, largest):
    gain = 1.0
    for dim, shards_of in pieces:
        steps = jax.random.uniform(jax.random.fold_in(jax.random.fold_in(key, 6), dim), (shards_of,), jnp.float32, least / len(pieces), largest / len(pieces))
        gain = gain * jnp.repeat(jnp.exp(steps), shape[dim] // shards_of).reshape((-1,) + (1,) * (len(shape) - 1 - dim))
    return gain


def normal_values(own_key, dims, scale, reach, cuts=(), dtype=jnp.bfloat16):
    level = block_scale(own_key, dims, cuts, -0.22, 0.18) if cuts else 1.0
    result = jax.random.normal(own_key, dims, jnp.float32) * scale * level
    return jnp.minimum(jnp.maximum(result, -reach), reach).astype(dtype)


def heavy_noise(stream_key, dims, scale, limit, cuts, heavy, dtype=jnp.bfloat16):
    values = scale * jax.random.normal(stream_key, dims, jnp.float32)
    if cuts:
        values = values * block_scale(stream_key, dims, cuts, -0.22, 0.18)
    return jnp.clip(strengthened(values, jax.random.fold_in(stream_key, 3), *heavy), -limit, limit).astype(dtype)


def setup_inputs(seed: int = 0) -> dict:
    key_of = jax.random.split(jax.random.key(seed), 7)
    design = heavy_noise(key_of[0], (NROWS, P_SIZE), 1.0, 24.0, ((0, 128),), (0, 1, 128, 5.5))
    observed = normal_values(key_of[1], (NROWS,), 1.0, 6.0, ((0, 128),), jnp.float32)
    weight_class = set_ends(jax.random.randint(key_of[2], (NROWS,), 0, CLASSES), jax.random.fold_in(key_of[2], 1), 0, CLASSES - 1).astype(jnp.int32)
    calib_unit = set_ends(jax.random.randint(key_of[3], (NROWS,), 0, UNITS), jax.random.fold_in(key_of[3], 1), 0, UNITS - 1).astype(jnp.int32)
    class_weight = jnp.clip(jnp.exp(jax.random.uniform(key_of[4], (CLASSES,), jnp.float32, math.log(0.5), math.log(8.0))), 0.5, 8.0)
    calib_scale = jnp.clip(jnp.exp(jax.random.uniform(key_of[5], (UNITS, NB), jnp.float32, math.log(0.5), math.log(2.0))), 0.5, 2.0)
    return dict(design=design, observed=observed, weight_class=weight_class, calib_unit=calib_unit, class_weight=class_weight, calib_scale=calib_scale)


def reference(design, observed, weight_class, calib_unit, class_weight, calib_scale):
    shards = NROWS // ROW_DEV
    design_b = design.reshape(shards, ROW_DEV, P_SIZE)
    observed_b = observed.reshape(shards, ROW_DEV)
    class_b = weight_class.reshape(shards, ROW_DEV)
    unit_b = calib_unit.reshape(shards, ROW_DEV)

    def step(carry, items):
        gram, rhs, chi = carry
        block, obs, cls, unit = items
        row_weight = class_weight[cls]
        root_weight = jnp.sqrt(row_weight)
        scales = jnp.repeat(calib_scale[unit], CB, axis=1)
        scaled = (block.astype(jnp.float32) * scales).astype(jnp.bfloat16)
        weighted = (root_weight[:, None] * scaled.astype(jnp.float32)).astype(jnp.bfloat16)
        gram = gram + lax.dot_general(weighted, weighted, (((0,), (0,)), ((), ())), preferred_element_type=jnp.float32)
        weighted_obs = (root_weight * obs).astype(jnp.bfloat16)
        rhs = rhs + jnp.dot(weighted_obs, weighted, preferred_element_type=jnp.float32)
        chi = chi + jnp.sum(row_weight * obs * obs)
        return ((gram, rhs, chi), None)
    init = (jnp.zeros((P_SIZE, P_SIZE), jnp.float32), jnp.zeros((P_SIZE,), jnp.float32), jnp.zeros((), jnp.float32))
    (gram, rhs, chi), unused = lax.scan(step, init, (design_b, observed_b, class_b, unit_b))
    return (gram / NROWS, rhs / NROWS, chi / NROWS)
```

```python
import functools

import jax
import jax.numpy as jnp
from jax import lax
from jax.experimental import pallas as pl
from jax.experimental.pallas import tpu as pltpu
from jax.sharding import PartitionSpec as P

F32 = jnp.float32
BF16 = jnp.bfloat16
ROWS = 3072
WIDTH = 1024
BLOCKS = 8
LANES = 128
UNITS = 64
CLASSES = 16
CHUNK = 256
CHUNKS = ROWS // CHUNK
TILE = 72
PART = 24
TOTAL = 393216.0
OFFSETS = (2, 1, 3, 0)
NT = (((1,), (1,)), ((), ()))
MESH = pl.DeviceIdType.MESH


def part_rows(part):
    return pl.ds(PART * part, PART)


def kernel(
    design, observed, weight_class, calib_unit, class_weight, scale_t,
    out,
    dbuf, wt, row_scale, row_obs, own, other, arrived,
    ring_x, ring_z, ring_y, ring_2, last,
    load_sem, send_sem, recv_sem,
):
    r = lax.axis_index("rows")
    g = lax.axis_index("grid")
    z, x, y, c = r // 4, r % 4, g // 2, g % 2

    for q in range(CHUNKS):
        rows = pl.ds(q * CHUNK, CHUNK)
        pltpu.make_async_copy(design.at[rows], dbuf.at[rows], load_sem.at[q]).start()

    def device(dz=0, dx=0, dy=0, flip=False):
        core = 1 - c if flip else c
        return (4 * ((z + dz) % 4) + (x + dx) % 4, 2 * ((y + dy) % 4) + core)

    partner = device(flip=True)
    axis_device = {
        "x": lambda d: device(dx=d),
        "z": lambda d: device(dz=d),
        "y": lambda d: device(dy=d),
    }
    barrier = pltpu.get_barrier_semaphore()
    peers = [partner] + [axis_device[a](d) for a in "xzy" for d in (1, 2, 3)]
    for peer in peers:
        pl.semaphore_signal(barrier, inc=1, device_id=peer, device_id_type=MESH)

    started = []

    def send(src, dst, peer):
        index = len(started)
        copy = pltpu.make_async_remote_copy(
            src_ref=src, dst_ref=dst, send_sem=send_sem.at[index],
            recv_sem=recv_sem.at[index], device_id=peer, device_id_type=MESH,
        )
        copy.start()
        started.append(copy)
        return copy

    classes = weight_class[...]
    row_weight = jnp.zeros(classes.shape, F32)
    for k in range(CLASSES):
        row_weight = jnp.where(classes == k, class_weight[k], row_weight)
    root = jnp.sqrt(row_weight)
    obs = observed[...]
    chi = jnp.sum(row_weight * obs * obs)
    root_obs = root * obs
    unit_id = lax.broadcasted_iota(jnp.int32, (UNITS, LANES), 0)
    scales = scale_t[...]
    for q in range(ROWS // LANES):
        cols = slice(q * LANES, (q + 1) * LANES)
        hot = (unit_id == calib_unit[q : q + 1, :]).astype(F32)
        scale = jnp.dot(scales, hot, precision=lax.Precision.HIGHEST, preferred_element_type=F32)
        scale = scale * root[q : q + 1, :]
        row_scale[:, cols] = scale
        value = scale * root_obs[q : q + 1, :]
        high = value.astype(BF16)
        low = (value - high.astype(F32)).astype(BF16)
        row_obs[:, cols] = jnp.concatenate([high, low], axis=0)

    def block_at(position):
        group, a = position // 2, position % 2
        k = 2 * (group // 2) + a
        core = c if group % 2 else 1 - c
        return (y + OFFSETS[k]) % 4, core

    def load_chunk(q, acc):
        rows = pl.ds(pl.multiple_of(q * CHUNK, CHUNK), CHUNK)
        pltpu.make_async_copy(design.at[rows], dbuf.at[rows], load_sem.at[q]).wait()
        for position in range(BLOCKS):
            high, core = block_at(position)
            block = 2 * high + core
            cols = pl.ds(pl.multiple_of(block * LANES, LANES), LANES)
            piece = dbuf[rows, cols].T.astype(F32)
            wt[position, :, rows] = (piece * row_scale[pl.ds(block, 1), rows]).astype(BF16)
        return acc + jnp.dot(row_obs[:, rows], dbuf[rows, :], preferred_element_type=F32)

    sums = lax.fori_loop(0, CHUNKS, load_chunk, jnp.zeros((2 * BLOCKS, WIDTH), F32))
    sums = sums[:BLOCKS] + sums[BLOCKS:]
    line = lax.broadcasted_iota(jnp.int32, (8, LANES), 0)
    for block in range(BLOCKS):
        rhs = sums[block : block + 1, block * LANES : (block + 1) * LANES]
        extra = jnp.where(line == 0, rhs, jnp.where(line == 1, chi, 0.0))
        for k in range(4):
            for half in range(2):
                strip = 2 * (block % 2) + half
                own[k, block // 2, strip, 64:72, :] = extra
                other[k, block // 2, strip, 64:72, :] = extra

    def store(row_position, col_position, value):
        group, a = col_position // 2, col_position % 2
        target = own if group % 2 else other
        k = 2 * (group // 2) + a
        high, core = block_at(row_position)
        for half in range(2):
            target[k, high, 2 * core + half, 0:64, :] = value[64 * half : 64 * half + 64]

    def panel(group):
        right = wt[2 * group : 2 * group + 2].reshape(2 * LANES, ROWS)
        count = BLOCKS - 2 * group
        left = wt[2 * group : BLOCKS].reshape(count * LANES, ROWS)
        product = lax.dot_general(left, right, NT, preferred_element_type=F32)
        for i in range(count):
            for a in range(2):
                value = product[i * LANES : (i + 1) * LANES, a * LANES : (a + 1) * LANES]
                store(2 * group + i, 2 * group + a, value)
                if i >= 2:
                    store(2 * group + a, 2 * group + i, value.T)

    def exchange(pair):
        return [send(other.at[k], arrived.at[k], partner) for k in (2 * pair, 2 * pair + 1)]

    def merge(pair, copies):
        for copy in copies:
            copy.wait_recv()
        for k in (2 * pair, 2 * pair + 1):
            def add(i, _):
                own[k, i // 4, i % 4] = own[k, i // 4, i % 4] + arrived[k, i // 4, i % 4]
                return 0
            lax.fori_loop(0, 16, add, 0)

    class Ring:
        def __init__(self, axis, src, bufs):
            self.right, self.left = axis_device[axis](1), axis_device[axis](3)
            self.src, self.bufs = src, bufs

        def start_far(self):
            self.hop_a = send(self.src(2, 0), self.bufs[0], self.right)
            self.hop_b = send(self.src(2, 1), self.bufs[1], self.left)

        def start_right(self):
            self.direct_b = send(self.src(1, 1), self.bufs[3], self.right)

        def start_left(self):
            self.direct_a = send(self.src(3, 0), self.bufs[2], self.left)

        def mid_a(self):
            self.hop_a.wait_recv()
            self.bufs[0][...] = self.bufs[0][...] + self.src(1, 0)[...]
            self.last_a = send(self.bufs[0], self.bufs[4], self.right)

        def mid_b(self):
            self.hop_b.wait_recv()
            self.bufs[1][...] = self.bufs[1][...] + self.src(3, 1)[...]
            self.last_b = send(self.bufs[1], self.bufs[5], self.left)

        def start(self):
            self.start_far()
            self.start_right()
            self.start_left()

        def mid(self):
            self.mid_a()
            self.mid_b()

        def finish(self):
            self.direct_a.wait_recv()
            self.last_a.wait_recv()
            mine = self.src(0, 0)
            mine[...] = mine[...] + self.bufs[2][...] + self.bufs[4][...]
            self.direct_b.wait_recv()
            self.last_b.wait_recv()
            mine = self.src(0, 1)
            mine[...] = mine[...] + self.bufs[3][...] + self.bufs[5][...]

    panel_of = {2: 0, 1: 1, 3: 2, 0: 3}

    def first_x(pair):
        def src(d, half):
            return own.at[2 * pair + half, :, (x + d) % 4, part_rows(0), :]
        return Ring("x", src, [ring_x.at[pair, i] for i in range(6)])

    def first_z(pair):
        def src(d, half):
            return own.at[2 * pair + half, (z + d) % 4, :, part_rows(2), :]
        return Ring("z", src, [ring_z.at[pair, i] for i in range(6)])

    def first_y():
        def src(d, half):
            return own.at[panel_of[d], pl.ds(2 * half, 2), :, part_rows(1), :]
        return Ring("y", src, [ring_y.at[i] for i in range(6)])

    def second(part):
        def src(d, half):
            two = pl.ds(2 * half, 2)
            if part == 0:
                return own.at[panel_of[d], two, x, part_rows(0), :]
            if part == 1:
                return own.at[3, (z + d) % 4, two, part_rows(1), :]
            return own.at[two, z, (x + d) % 4, part_rows(2), :]
        return Ring("yzx"[part], src, [ring_2.at[part, i] for i in range(6)])

    def third_src(part, d):
        if part == 0:
            return own.at[3, (z + d) % 4, x, part_rows(0), :]
        if part == 1:
            return own.at[3, z, (x + d) % 4, part_rows(1), :]
        return own.at[panel_of[d], z, x, part_rows(2), :]

    def third(part):
        to = axis_device["zxy"[part]]
        return [send(third_src(part, d), last.at[part, d - 1], to(d)) for d in (2, 1, 3)]

    def third_finish(part, copies):
        for copy in copies:
            copy.wait_recv()
        total = third_src(part, 0)[...] + last[part, 0] + last[part, 1] + last[part, 2]
        out[part_rows(part), :] = total * (1.0 / TOTAL)

    pl.semaphore_wait(barrier, len(peers))
    panel(0)
    pair_0 = exchange(0)
    panel(1)
    merge(0, pair_0)
    x_0, z_0, y_all = first_x(0), first_z(0), first_y()
    x_0.start()
    z_0.start()
    y_all.start_far()
    y_all.start_right()
    panel(2)
    pair_1 = exchange(1)
    panel(3)
    merge(1, pair_1)
    x_1, z_1 = first_x(1), first_z(1)
    x_1.start()
    z_1.start()
    y_all.start_left()
    x_0.mid()
    z_0.mid()
    y_all.mid()
    x_1.mid()
    z_1.mid()
    rings = [second(part) for part in range(3)]
    y_all.finish()
    rings[1].start()
    x_0.finish()
    x_1.finish()
    rings[0].start()
    z_0.finish()
    z_1.finish()
    rings[2].start()
    for part in (1, 0, 2):
        rings[part].mid()
    tails = {}
    for part in (1, 0, 2):
        rings[part].finish()
        tails[part] = third(part)
    for part in (1, 0, 2):
        third_finish(part, tails[part])
    for copy in started:
        copy.wait_send()


COPIES = 4 + 12 + 12 + 6 + 18 + 9


def local(design, observed, weight_class, calib_unit, class_weight, calib_scale):
    dense = (ROWS // LANES, LANES)
    vmem = pl.BlockSpec(memory_space=pltpu.VMEM)
    panels = pltpu.VMEM((4, 4, 4, TILE, LANES), F32)
    tile = pl.pallas_call(
        kernel,
        out_shape=jax.ShapeDtypeStruct((TILE, LANES), F32),
        in_specs=[pl.BlockSpec(memory_space=pl.ANY), vmem, vmem, vmem,
                  pl.BlockSpec(memory_space=pltpu.SMEM), vmem],
        out_specs=vmem,
        scratch_shapes=[
            pltpu.VMEM((ROWS, WIDTH), BF16),
            pltpu.VMEM((BLOCKS, LANES, ROWS), BF16),
            pltpu.VMEM((BLOCKS, ROWS), F32),
            pltpu.VMEM((2 * BLOCKS, ROWS), BF16),
            panels, panels, panels,
            pltpu.VMEM((2, 6, 4, PART, LANES), F32),
            pltpu.VMEM((2, 6, 4, PART, LANES), F32),
            pltpu.VMEM((6, 2, 4, PART, LANES), F32),
            pltpu.VMEM((3, 6, 2, PART, LANES), F32),
            pltpu.VMEM((3, 3, PART, LANES), F32),
            pltpu.SemaphoreType.DMA((CHUNKS,)),
            pltpu.SemaphoreType.DMA((COPIES,)),
            pltpu.SemaphoreType.DMA((COPIES,)),
        ],
        compiler_params=pltpu.CompilerParams(
            collective_id=0, has_side_effects=True, vmem_limit_bytes=56 * 2**20
        ),
    )(
        design,
        observed.reshape(dense),
        weight_class.reshape(dense),
        calib_unit.reshape(dense),
        class_weight,
        calib_scale.T,
    )
    row, col = lax.axis_index("rows"), lax.axis_index("grid")
    right_hand = lax.dynamic_slice(tile, (64, 64 * (row % 2) + 8 * col), (1, 8)).reshape(8)
    return tile[:64], right_hand, tile[65, 0]


def solution(mesh):
    both = ("rows", "grid")
    return jax.shard_map(
        local,
        mesh=mesh,
        in_specs=(P(both, None), P(both), P(both), P(both), P(), P()),
        out_specs=(P("rows", "grid"), P(both), P()),
        check_vma=False,
    )
```

```python
import functools

import jax
import jax.numpy as jnp
from jax import lax
from jax.experimental import pallas as pl
from jax.experimental.pallas import tpu as pltpu
from jax.sharding import PartitionSpec as P

F32 = jnp.float32
BF16 = jnp.bfloat16
ROWS = 3072
WIDTH = 1024
BLOCKS = 8
LANES = 128
UNITS = 64
CLASSES = 16
CHUNK = 256
CHUNKS = ROWS // CHUNK
TILE = 64
STEP = 1024
PARTS = ((0, 24), (24, 16), (40, 24))
EXTRA = 16
TOTAL = 393216.0
OFFSETS = (2, 1, 3, 0)
NT = (((1,), (1,)), ((), ()))
MESH = pl.DeviceIdType.MESH


def part_rows(part):
    return pl.ds(*PARTS[part])


def kernel(
    design, observed_in, class_in, unit_in, weight_in, scale_in,
    out, out_extra,
    dbuf, wt, row_scale, row_obs, own, other, arrived, partial,
    first_xz, first_y, second_0, second_1, second_2, last_0, last_1, last_2,
    extra_core, extra_ring,
    observed, weight_class, calib_unit, class_weight, scale_t,
    load_sem, small_sem, send_sem, recv_sem,
):
    r = lax.axis_index("rows")
    g = lax.axis_index("grid")
    z, x, y, c = r // 4, r % 4, g // 2, g % 2

    small = [
        pltpu.make_async_copy(src, dst, small_sem.at[i])
        for i, (src, dst) in enumerate([
            (class_in, weight_class), (weight_in, class_weight), (observed_in, observed),
            (unit_in, calib_unit), (scale_in, scale_t),
        ])
    ]
    for copy in small:
        copy.start()
    for q in range(CHUNKS):
        rows = pl.ds(q * CHUNK, CHUNK)
        pltpu.make_async_copy(design.at[rows], dbuf.at[rows], load_sem.at[q]).start()

    def device(dz=0, dx=0, dy=0, flip=False):
        core = 1 - c if flip else c
        return (4 * ((z + dz) % 4) + (x + dx) % 4, 2 * ((y + dy) % 4) + core)

    partner = device(flip=True)
    axis_device = {
        "x": lambda d: device(dx=d),
        "z": lambda d: device(dz=d),
        "y": lambda d: device(dy=d),
    }
    barrier = pltpu.get_barrier_semaphore()
    peers = [partner] + [axis_device[a](d) for a in "xzy" for d in (1, 2, 3)]
    for peer in peers:
        pl.semaphore_signal(barrier, inc=1, device_id=peer, device_id_type=MESH)

    started = []

    def send(src, dst, peer):
        index = len(started)
        copy = pltpu.make_async_remote_copy(
            src_ref=src, dst_ref=dst, send_sem=send_sem.at[index],
            recv_sem=recv_sem.at[index], device_id=peer, device_id_type=MESH,
        )
        copy.start()
        started.append(copy)
        return copy

    for copy in small:
        copy.wait()
    classes = weight_class[...]
    row_weight = jnp.zeros(classes.shape, F32)
    for k in range(CLASSES):
        row_weight = jnp.where(classes == k, class_weight[k], row_weight)
    root = jnp.sqrt(row_weight)
    obs = observed[...]
    extra_core[c] = jnp.zeros((EXTRA, LANES), F32) + jnp.sum(row_weight * obs * obs)
    root_obs = root * obs
    unit_id = lax.broadcasted_iota(jnp.int32, (UNITS, LANES), 0)
    scales = scale_t[...]
    obs_line = lax.broadcasted_iota(jnp.int32, (EXTRA, LANES), 0)
    for q in range(ROWS // LANES):
        cols = slice(q * LANES, (q + 1) * LANES)
        hot = (unit_id == calib_unit[q : q + 1, :]).astype(F32)
        scale = jnp.dot(scales, hot, precision=lax.Precision.HIGHEST, preferred_element_type=F32)
        scale = scale * root[q : q + 1, :]
        row_scale[:, cols] = scale
        value = root_obs[q : q + 1, :]
        high = value.astype(BF16).astype(F32)
        both = jnp.where(obs_line == 0, high, jnp.where(obs_line == 1, value - high, 0.0))
        row_obs[:, cols] = both.astype(BF16)

    def block_at(position):
        core = c if position % 2 else 1 - c
        return (y + OFFSETS[position // 2]) % 4, core

    def weigh(q):
        rows = pl.ds(q * CHUNK, CHUNK)
        pltpu.make_async_copy(design.at[rows], dbuf.at[rows], load_sem.at[q]).wait()
        for position in range(BLOCKS):
            high, core = block_at(position)
            block = 2 * high + core
            cols = pl.ds(pl.multiple_of(block * LANES, LANES), LANES)
            piece = dbuf[rows, cols].T.astype(F32)
            wt[position, :, rows] = (piece * row_scale[pl.ds(block, 1), rows]).astype(BF16)

    def store(row_position, col_position, value):
        target = own if col_position % 2 else other
        high, core = block_at(row_position)
        for half in range(2):
            target[col_position // 2, high, 2 * core + half] = value[64 * half : 64 * half + 64]

    def multiply(i, j, cols):
        count = ROWS if cols == slice(None) else STEP
        left = wt[2 * i : 2 * i + 2, :, cols].reshape(2 * LANES, count)
        if i == j:
            left = jnp.concatenate([left, row_obs[:, cols]], axis=0)
        right = wt[2 * j : 2 * j + 2, :, cols].reshape(2 * LANES, count)
        return lax.dot_general(left, right, NT, preferred_element_type=F32)

    def keep(i, j, product):
        for a in range(2):
            for b in range(2):
                value = product[a * LANES : (a + 1) * LANES, b * LANES : (b + 1) * LANES]
                store(2 * i + a, 2 * j + b, value)
                if i > j:
                    store(2 * j + b, 2 * i + a, value.T)
        if i == j:
            line = 2 * LANES
            rhs = product[line : line + 1] + product[line + 1 : line + 2]
            for b in range(2):
                high, core = block_at(2 * j + b)
                extra_core[c, pl.ds(2 * high + core, 1), :] = rhs[:, b * LANES : (b + 1) * LANES]

    def square(i, j):
        keep(i, j, multiply(i, j, slice(None)))

    def panel(k):
        for i in range(k, 4):
            square(i, k)

    def first_panel(step):
        cols = slice(step * STEP, (step + 1) * STEP)
        for i in range(4):
            product = multiply(i, 0, cols)
            lines = product.shape[0]
            if step:
                product = product + partial[i, :lines]
            if (step + 1) * STEP < ROWS:
                partial[i, :lines] = product
            else:
                keep(i, 0, product)

    def exchange(k):
        return send(other.at[k], arrived.at[k], partner)

    def merge(k, copy):
        copy.wait_recv()

        def add(i, _):
            own[k, i] = own[k, i] + arrived[k, i]
            return 0

        lax.fori_loop(0, 4, add, 0)

    def scatter(axis, src, bufs):
        to = axis_device[axis]
        return [(send(src(d), bufs.at[d - 1], to(d)), bufs.at[d - 1]) for d in (2, 1, 3)]

    def gather(src, copies):
        for copy, _ in copies:
            copy.wait_recv()
        mine = src(0)
        total = mine[...]
        for _, buf in copies:
            total = total + buf[...]
        mine[...] = total

    panel_of = {2: 0, 1: 1, 3: 2, 0: 3}

    def at(part, k, dz, dx):
        return own.at[k, dz, dx, part_rows(part), :]

    every = slice(None)

    def src_x(k):
        return lambda d: at(0, k, every, (x + d) % 4)

    def src_z(k):
        return lambda d: at(2, k, (z + d) % 4, every)

    def src_y(d):
        return at(1, panel_of[d], every, every)

    def src_0y(d):
        return at(0, panel_of[d], every, x)

    def src_1z(d):
        return at(1, 3, (z + d) % 4, every)

    def src_2x(k):
        return lambda d: at(2, k, z, (x + d) % 4)

    def src_0z(d):
        return at(0, 3, (z + d) % 4, x)

    def src_1x(d):
        return at(1, 3, z, (x + d) % 4)

    def src_2y(d):
        return at(2, panel_of[d], z, x)

    to_y = axis_device["y"]
    distance_of = (2, 1, 3, 0)
    step_x, step_z, step_y, step_0y, step_2x, step_2y = {}, {}, [], [], {}, []

    def spread(k):
        step_x[k] = scatter("x", src_x(k), first_xz.at[0, k])
        step_z[k] = scatter("z", src_z(k), first_xz.at[1, k])
        if k < 3:
            d = distance_of[k]
            step_y.append((send(src_y(d), first_y.at[k], to_y(d)), first_y.at[k]))

    def gather_extra(stage, copies):
        for copy in copies:
            copy.wait_recv()
        total = extra_ring[stage, 0] + extra_ring[stage, 1]
        return total + extra_ring[stage, 2] + extra_ring[stage, 3]

    def spread_extra(stage, total):
        place = (x, y, z)[stage]
        to = axis_device["xyz"[stage]]
        extra_ring[stage, place] = total
        slot = extra_ring.at[stage, place]
        return [send(slot, slot, to(d)) for d in (2, 1, 3)]

    per_step = STEP // CHUNK
    for step in range(ROWS // STEP + 1):
        if step < ROWS // STEP:
            for q in range(step * per_step, (step + 1) * per_step):
                weigh(q)
        if step:
            first_panel(step - 1)
    pl.semaphore_wait(barrier, len(peers))
    sent_0 = exchange(0)
    panel(1)
    sent_1 = exchange(1)
    panel(2)
    sent_2 = exchange(2)
    merge(0, sent_0)
    spread(0)
    panel(3)
    sent_3 = exchange(3)
    slot = extra_core.at[c]
    sent_extra = send(slot, slot, partner)
    for k, copy in ((1, sent_1), (2, sent_2), (3, sent_3)):
        merge(k, copy)
        spread(k)
    sent_extra.wait_recv()
    extra = spread_extra(0, extra_core[0] + extra_core[1])
    for k in range(4):
        gather(src_x(k), step_x[k])
        if k < 3:
            d = distance_of[k]
            step_0y.append((send(src_0y(d), second_0.at[k], to_y(d)), second_0.at[k]))
        gather(src_z(k), step_z[k])
        step_2x[k] = scatter("x", src_2x(k), second_2.at[k])
    extra = spread_extra(1, gather_extra(0, extra))
    gather(src_y, step_y)
    step_1z = scatter("z", src_1z, second_1)
    gather(src_0y, step_0y)
    step_0z = scatter("z", src_0z, last_0)
    for k in range(4):
        gather(src_2x(k), step_2x[k])
        if k < 3:
            d = distance_of[k]
            step_2y.append((send(src_2y(d), last_2.at[k], to_y(d)), last_2.at[k]))
    extra = spread_extra(2, gather_extra(1, extra))
    gather(src_1z, step_1z)
    step_1x = scatter("x", src_1x, last_1)
    for part, src, copies in ((0, src_0z, step_0z), (2, src_2y, step_2y), (1, src_1x, step_1x)):
        for copy, _ in copies:
            copy.wait_recv()
        total = src(0)[...]
        for _, buf in copies:
            total = total + buf[...]
        out[part_rows(part), :] = total * (1.0 / TOTAL)
    out_extra[...] = gather_extra(2, extra) * (1.0 / TOTAL)
    for copy in started:
        copy.wait_send()


COPIES = 4 + 12 + 12 + 3 + 3 + 3 + 12 + 9 + 10


def local(design, observed, weight_class, calib_unit, class_weight, calib_scale):
    dense = (ROWS // LANES, LANES)
    vmem = pl.BlockSpec(memory_space=pltpu.VMEM)
    panels = pltpu.VMEM((4, 4, 4, TILE, LANES), F32)
    rows_x, rows_y, rows_z = (rows for _, rows in PARTS)
    gram, extra = pl.pallas_call(
        kernel,
        out_shape=(jax.ShapeDtypeStruct((TILE, LANES), F32), jax.ShapeDtypeStruct((EXTRA, LANES), F32)),
        in_specs=[pl.BlockSpec(memory_space=pltpu.HBM)] * 6,
        out_specs=(vmem, vmem),
        scratch_shapes=[
            pltpu.VMEM((ROWS, WIDTH), BF16),
            pltpu.VMEM((BLOCKS, LANES, ROWS), BF16),
            pltpu.VMEM((BLOCKS, ROWS), F32),
            pltpu.VMEM((EXTRA, ROWS), BF16),
            panels, panels, panels,
            pltpu.VMEM((4, 2 * LANES + EXTRA, 2 * LANES), F32),
            pltpu.VMEM((2, 4, 3, 4, rows_x, LANES), F32),
            pltpu.VMEM((3, 4, 4, rows_y, LANES), F32),
            pltpu.VMEM((3, 4, rows_x, LANES), F32),
            pltpu.VMEM((3, 4, rows_y, LANES), F32),
            pltpu.VMEM((4, 3, rows_z, LANES), F32),
            pltpu.VMEM((3, rows_x, LANES), F32),
            pltpu.VMEM((3, rows_y, LANES), F32),
            pltpu.VMEM((3, rows_z, LANES), F32),
            pltpu.VMEM((2, EXTRA, LANES), F32),
            pltpu.VMEM((3, 4, EXTRA, LANES), F32),
            pltpu.VMEM(dense, F32),
            pltpu.VMEM(dense, jnp.int32),
            pltpu.VMEM(dense, jnp.int32),
            pltpu.SMEM((CLASSES,), F32),
            pltpu.VMEM((BLOCKS, UNITS), F32),
            pltpu.SemaphoreType.DMA((CHUNKS,)),
            pltpu.SemaphoreType.DMA((5,)),
            pltpu.SemaphoreType.DMA((COPIES,)),
            pltpu.SemaphoreType.DMA((COPIES,)),
        ],
        compiler_params=pltpu.CompilerParams(
            collective_id=0, has_side_effects=True, vmem_limit_bytes=32 * 2**20
        ),
    )(
        *[pltpu.with_memory_space_constraint(v, pltpu.HBM) for v in (design,
        observed.reshape(dense),
        weight_class.reshape(dense),
        calib_unit.reshape(dense),
        class_weight,
        calib_scale.T)],
    )
    row, col = lax.axis_index("rows"), lax.axis_index("grid")
    right_hand = lax.dynamic_slice(extra, (row // 2, 64 * (row % 2) + 8 * col), (1, 8)).reshape(8)
    return gram, right_hand, extra[BLOCKS, 0]


def solution(mesh):
    both = ("rows", "grid")
    return jax.shard_map(
        local,
        mesh=mesh,
        in_specs=(P(both, None), P(both), P(both), P(both), P(), P()),
        out_specs=(P("rows", "grid"), P(both), P()),
        check_vma=False,
    )
```

```python
import functools

import jax
import jax.numpy as jnp
from jax import lax
from jax.experimental import pallas as pl
from jax.experimental.pallas import tpu as pltpu
from jax.sharding import PartitionSpec as P

F32 = jnp.float32
BF16 = jnp.bfloat16
ROWS = 3072
WIDTH = 1024
BLOCKS = 8
LANES = 128
UNITS = 64
CLASSES = 16
LOADS = ((0, 512), (512, 1280), (1792, 1280))
CHUNKS = len(LOADS)
TILE = 64
PARTS = ((0, 24), (24, 16), (40, 24))
RINGS = 3
EXTRA = 16
TOTAL = 393216.0
OFFSETS = (2, 1, 3, 0)
NT = (((1,), (1,)), ((), ()))
MESH = pl.DeviceIdType.MESH


def part_rows(part):
    return pl.ds(*PARTS[part])


def kernel(
    design, observed_in, class_in, unit_in, weight_in, scale_in,
    out, out_extra,
    dbuf, wt, row_scale, row_obs, own, other, arrived, partial,
    ring_x, ring_z, ring_y, first_x, first_z, second_0, second_1, second_2, last_0, last_1, last_2,
    extra_core, extra_ring,
    observed, weight_class, calib_unit, class_weight, scale_t,
    load_sem, small_sem, send_sem, recv_sem,
):
    r = lax.axis_index("rows")
    g = lax.axis_index("grid")
    z, x, y, c = r // 4, r % 4, g // 2, g % 2

    small = [
        pltpu.make_async_copy(src, dst, small_sem.at[i])
        for i, (src, dst) in enumerate([
            (class_in, weight_class), (weight_in, class_weight), (observed_in, observed),
            (unit_in, calib_unit), (scale_in, scale_t),
        ])
    ]
    for copy in small:
        copy.start()
    for q in range(CHUNKS):
        rows = pl.ds(*LOADS[q])
        pltpu.make_async_copy(design.at[rows], dbuf.at[rows], load_sem.at[q]).start()

    def device(dz=0, dx=0, dy=0, flip=False):
        core = 1 - c if flip else c
        return (4 * ((z + dz) % 4) + (x + dx) % 4, 2 * ((y + dy) % 4) + core)

    partner = device(flip=True)
    axis_device = {
        "x": lambda d: device(dx=d),
        "z": lambda d: device(dz=d),
        "y": lambda d: device(dy=d),
    }
    barrier = pltpu.get_barrier_semaphore()
    peers = [partner] + [axis_device[a](d) for a in "xzy" for d in (1, 2, 3)]
    for peer in peers:
        pl.semaphore_signal(barrier, inc=1, device_id=peer, device_id_type=MESH)

    started = []

    def prepare(src, dst, peer):
        index = len(started)
        copy = pltpu.make_async_remote_copy(
            src_ref=src, dst_ref=dst, send_sem=send_sem.at[index],
            recv_sem=recv_sem.at[index], device_id=peer, device_id_type=MESH,
        )
        started.append(copy)
        return copy

    def send(src, dst, peer):
        copy = prepare(src, dst, peer)
        copy.start()
        return copy

    for copy in small:
        copy.wait()
    classes = weight_class[...]
    row_weight = jnp.zeros(classes.shape, F32)
    for k in range(CLASSES):
        row_weight = jnp.where(classes == k, class_weight[k], row_weight)
    root = jnp.sqrt(row_weight)
    obs = observed[...]
    extra_core[c] = jnp.zeros((EXTRA, LANES), F32) + jnp.sum(row_weight * obs * obs)
    root_obs = root * obs
    unit_id = lax.broadcasted_iota(jnp.int32, (UNITS, LANES), 0)
    scales = scale_t[...]
    parts = []
    for _ in range(3):
        parts.append(scales.astype(BF16).astype(F32))
        scales = scales - parts[-1]
    scales = jnp.concatenate(parts, axis=0).astype(BF16)
    obs_line = lax.broadcasted_iota(jnp.int32, (EXTRA, LANES), 0)
    for q in range(ROWS // LANES):
        cols = slice(q * LANES, (q + 1) * LANES)
        hot = jnp.where(unit_id == calib_unit[q : q + 1, :], 1.0, 0.0).astype(BF16)
        triple = jnp.dot(scales, hot, preferred_element_type=F32)
        scale = triple[:BLOCKS] + triple[BLOCKS : 2 * BLOCKS] + triple[2 * BLOCKS :]
        scale = scale * root[q : q + 1, :]
        row_scale[:, cols] = scale
        value = root_obs[q : q + 1, :]
        high = value.astype(BF16).astype(F32)
        both = jnp.where(obs_line == 0, high, jnp.where(obs_line == 1, value - high, 0.0))
        row_obs[:, cols] = both.astype(BF16)

    def block_at(position):
        core = c if position % 2 else 1 - c
        return (y + OFFSETS[position // 2]) % 4, core

    def weigh(q):
        rows = pl.ds(*LOADS[q])
        pltpu.make_async_copy(design.at[rows], dbuf.at[rows], load_sem.at[q]).wait()
        for position in range(BLOCKS):
            high, core = block_at(position)
            block = 2 * high + core
            cols = pl.ds(pl.multiple_of(block * LANES, LANES), LANES)
            piece = dbuf[rows, cols].T.astype(F32)
            wt[position, :, rows] = (piece * row_scale[pl.ds(block, 1), rows]).astype(BF16)

    def store(row_position, col_position, value):
        target = own if col_position % 2 else other
        high, core = block_at(row_position)
        for half in range(2):
            target[col_position // 2, high, 2 * core + half] = value[64 * half : 64 * half + 64]

    squares = [(i, j) for j in range(4) for i in range(j, 4)]

    def multiply(i, j, step):
        start, count = LOADS[step]
        cols = slice(start, start + count)
        left = wt[2 * i : 2 * i + 2, :, cols].reshape(2 * LANES, count)
        if i == j:
            left = jnp.concatenate([left, row_obs[:, cols]], axis=0)
        right = wt[2 * j : 2 * j + 2, :, cols].reshape(2 * LANES, count)
        product = lax.dot_general(left, right, NT, preferred_element_type=F32)
        place, lines = squares.index((i, j)), product.shape[0]
        if step:
            product = product + partial[place, :lines]
        if step + 1 < CHUNKS:
            partial[place, :lines] = product
        else:
            keep(i, j, product)

    def keep(i, j, product):
        for a in range(2):
            for b in range(2):
                value = product[a * LANES : (a + 1) * LANES, b * LANES : (b + 1) * LANES]
                store(2 * i + a, 2 * j + b, value)
                if i > j:
                    store(2 * j + b, 2 * i + a, value.T)
        if i == j:
            line = 2 * LANES
            rhs = product[line : line + 1] + product[line + 1 : line + 2]
            for b in range(2):
                high, core = block_at(2 * j + b)
                extra_core[c, pl.ds(2 * high + core, 1), :] = rhs[:, b * LANES : (b + 1) * LANES]

    def panel(k, step=CHUNKS - 1):
        for i in range(k, 4):
            multiply(i, k, step)

    exchanged = {}

    def exchange(j):
        pairs = [(j, i) for i in range(j, 4)] + [(i, j) for i in range(j + 1, 4)]
        for k, i in pairs:
            line = (y + OFFSETS[i]) % 4
            exchanged[k, i] = send(other.at[k, line], arrived.at[k, line], partner)

    def merge(k):
        for i in range(4):
            exchanged[k, i].wait_recv()

        def add(i, _):
            own[k, i] = own[k, i] + arrived[k, i]
            return 0

        lax.fori_loop(0, 4, add, 0)

    def scatter(axis, src, bufs):
        to = axis_device[axis]
        return [(prepare(src(d), bufs.at[d - 1], to(d)), bufs.at[d - 1]) for d in (2, 1, 3)]

    def start(copies):
        for copy, _ in copies:
            copy.start()
        return copies

    def gather(src, copies):
        for copy, _ in copies:
            copy.wait_recv()
        mine = src(0)
        total = mine[...]
        for _, buf in copies:
            total = total + buf[...]
        mine[...] = total

    class Ring:
        def __init__(self, axis, src, bufs):
            right, left = axis_device[axis](1), axis_device[axis](3)
            self.src, self.bufs = src, bufs
            self.hop_a = prepare(src(2, 0), bufs.at[0], right)
            self.hop_b = prepare(src(2, 1), bufs.at[1], left)
            self.direct_b = prepare(src(1, 1), bufs.at[3], right)
            self.direct_a = prepare(src(3, 0), bufs.at[2], left)
            self.last_a = prepare(bufs.at[0], bufs.at[4], right)
            self.last_b = prepare(bufs.at[1], bufs.at[5], left)
            self.next_a, self.next_b = src(1, 0), src(3, 1)

        def start_far(self):
            self.hop_a.start()
            self.hop_b.start()

        def start_right(self):
            self.direct_b.start()

        def start_left(self):
            self.direct_a.start()

        def start(self):
            self.start_far()
            self.start_right()
            self.start_left()

        def pass_right(self):
            self.hop_a.wait_recv()
            self.bufs[0] = self.bufs[0] + self.next_a[...]
            self.last_a.start()

        def pass_left(self):
            self.hop_b.wait_recv()
            self.bufs[1] = self.bufs[1] + self.next_b[...]
            self.last_b.start()

        def finish(self):
            for half, direct, via in ((0, self.direct_a, self.last_a), (1, self.direct_b, self.last_b)):
                direct.wait_recv()
                via.wait_recv()
                mine = self.src(0, half)
                mine[...] = mine[...] + self.bufs[2 + half] + self.bufs[4 + half]

    panel_of = {2: 0, 1: 1, 3: 2, 0: 3}

    def at(part, k, dz, dx):
        return own.at[k, dz, dx, part_rows(part), :]

    every = slice(None)

    def two(half):
        return pl.ds(2 * half, 2)

    def half_x(k):
        return lambda d, half: at(0, k, two(half), (x + d) % 4)

    def half_z(k):
        return lambda d, half: at(2, k, (z + d) % 4, two(half))

    def half_y(d, half):
        return at(1, panel_of[d], two(half), every)

    def src_x(k):
        return lambda d: at(0, k, every, (x + d) % 4)

    def src_z(k):
        return lambda d: at(2, k, (z + d) % 4, every)

    def src_0y(d):
        return at(0, panel_of[d], every, x)

    def src_1z(d):
        return at(1, 3, (z + d) % 4, every)

    def src_2x(k):
        return lambda d: at(2, k, z, (x + d) % 4)

    def src_0z(d):
        return at(0, 3, (z + d) % 4, x)

    def src_1x(d):
        return at(1, 3, z, (x + d) % 4)

    def src_2y(d):
        return at(2, panel_of[d], z, x)

    to_y = axis_device["y"]
    distance_of = (2, 1, 3, 0)
    step_0y, step_2x, step_2y = [], {}, []
    rings = {k: (Ring("x", half_x(k), ring_x.at[k]), Ring("z", half_z(k), ring_z.at[k])) for k in range(RINGS)}
    ring_of_y = Ring("y", half_y, ring_y)

    step_x = {k: scatter("x", src_x(k), first_x.at[k - RINGS]) for k in range(RINGS, 4)}
    step_z = {k: scatter("z", src_z(k), first_z.at[k - RINGS]) for k in range(RINGS, 4)}

    def spread(k):
        if k < RINGS:
            for ring in rings[k]:
                ring.start()
        else:
            start(step_x[k])
            start(step_z[k])
        if k == 0:
            ring_of_y.start_far()
        if k == 1:
            ring_of_y.start_right()
        if k == 2:
            ring_of_y.start_left()

    def pass_on(k):
        for ring in rings[k]:
            ring.pass_right()
            ring.pass_left()

    def finish_x(k):
        if k < RINGS:
            rings[k][0].finish()
        else:
            gather(src_x(k), step_x[k])

    def finish_z(k):
        if k < RINGS:
            rings[k][1].finish()
        else:
            gather(src_z(k), step_z[k])

    def gather_extra(stage, copies):
        for copy in copies:
            copy.wait_recv()
        total = extra_ring[stage, 0] + extra_ring[stage, 1]
        return total + extra_ring[stage, 2] + extra_ring[stage, 3]

    def spread_extra(stage, total):
        place = (x, y, z)[stage]
        to = axis_device["xyz"[stage]]
        extra_ring[stage, place] = total
        slot = extra_ring.at[stage, place]
        return [send(slot, slot, to(d)) for d in (2, 1, 3)]

    weigh(0)
    for step in range(1, CHUNKS):
        weigh(step)
        for k in range(4):
            panel(k, step - 1)
    panel(0)
    pl.semaphore_wait(barrier, len(peers))
    exchange(0)
    panel(1)
    exchange(1)
    panel(2)
    exchange(2)
    panel(3)
    exchange(3)
    slot = extra_core.at[c]
    sent_extra = send(slot, slot, partner)
    merge(0)
    spread(0)
    merge(1)
    spread(1)
    merge(2)
    spread(2)
    pass_on(0)
    merge(3)
    spread(3)
    ring_of_y.pass_right()
    ring_of_y.pass_left()
    for k in range(1, RINGS):
        pass_on(k)
    sent_extra.wait_recv()
    extra = spread_extra(0, extra_core[0] + extra_core[1])
    for k in range(4):
        finish_x(k)
        if k < 3:
            d = distance_of[k]
            step_0y.append((send(src_0y(d), second_0.at[k], to_y(d)), second_0.at[k]))
        finish_z(k)
        step_2x[k] = start(scatter("x", src_2x(k), second_2.at[k]))
    extra = spread_extra(1, gather_extra(0, extra))
    ring_of_y.finish()
    step_1z = start(scatter("z", src_1z, second_1))
    gather(src_0y, step_0y)
    step_0z = start(scatter("z", src_0z, last_0))
    for k in range(4):
        gather(src_2x(k), step_2x[k])
        if k < 3:
            d = distance_of[k]
            step_2y.append((send(src_2y(d), last_2.at[k], to_y(d)), last_2.at[k]))
    extra = spread_extra(2, gather_extra(1, extra))
    gather(src_1z, step_1z)
    step_1x = start(scatter("x", src_1x, last_1))
    for part, src, copies in ((0, src_0z, step_0z), (2, src_2y, step_2y), (1, src_1x, step_1x)):
        for copy, _ in copies:
            copy.wait_recv()
        total = src(0)[...]
        for _, buf in copies:
            total = total + buf[...]
        out[part_rows(part), :] = total * (1.0 / TOTAL)
    out_extra[...] = gather_extra(2, extra) * (1.0 / TOTAL)
    for copy in started:
        copy.wait_send()


COPIES = 16 + 2 * (6 * RINGS + 3 * (4 - RINGS)) + 6 + 3 + 3 + 12 + 9 + 10


def local(design, observed, weight_class, calib_unit, class_weight, calib_scale):
    dense = (ROWS // LANES, LANES)
    vmem = pl.BlockSpec(memory_space=pltpu.VMEM)
    panels = pltpu.VMEM((4, 4, 4, TILE, LANES), F32)
    rows_x, rows_y, rows_z = (rows for _, rows in PARTS)
    gram, extra = pl.pallas_call(
        kernel,
        out_shape=(jax.ShapeDtypeStruct((TILE, LANES), F32), jax.ShapeDtypeStruct((EXTRA, LANES), F32)),
        in_specs=[pl.BlockSpec(memory_space=pltpu.HBM)] * 6,
        out_specs=(vmem, vmem),
        scratch_shapes=[
            pltpu.VMEM((ROWS, WIDTH), BF16),
            pltpu.VMEM((BLOCKS, LANES, ROWS), BF16),
            pltpu.VMEM((BLOCKS, ROWS), F32),
            pltpu.VMEM((EXTRA, ROWS), BF16),
            panels, panels, panels,
            pltpu.VMEM((10, 2 * LANES + EXTRA, 2 * LANES), F32),
            pltpu.VMEM((RINGS, 6, 2, rows_x, LANES), F32),
            pltpu.VMEM((RINGS, 6, 2, rows_z, LANES), F32),
            pltpu.VMEM((6, 2, 4, rows_y, LANES), F32),
            pltpu.VMEM((4 - RINGS, 3, 4, rows_x, LANES), F32),
            pltpu.VMEM((4 - RINGS, 3, 4, rows_z, LANES), F32),
            pltpu.VMEM((3, 4, rows_x, LANES), F32),
            pltpu.VMEM((3, 4, rows_y, LANES), F32),
            pltpu.VMEM((4, 3, rows_z, LANES), F32),
            pltpu.VMEM((3, rows_x, LANES), F32),
            pltpu.VMEM((3, rows_y, LANES), F32),
            pltpu.VMEM((3, rows_z, LANES), F32),
            pltpu.VMEM((2, EXTRA, LANES), F32),
            pltpu.VMEM((3, 4, EXTRA, LANES), F32),
            pltpu.VMEM(dense, F32),
            pltpu.VMEM(dense, jnp.int32),
            pltpu.VMEM(dense, jnp.int32),
            pltpu.SMEM((CLASSES,), F32),
            pltpu.VMEM((BLOCKS, UNITS), F32),
            pltpu.SemaphoreType.DMA((CHUNKS,)),
            pltpu.SemaphoreType.DMA((5,)),
            pltpu.SemaphoreType.DMA((COPIES,)),
            pltpu.SemaphoreType.DMA((COPIES,)),
        ],
        compiler_params=pltpu.CompilerParams(
            collective_id=0, has_side_effects=True, vmem_limit_bytes=32 * 2**20
        ),
    )(
        *[pltpu.with_memory_space_constraint(v, pltpu.HBM) for v in (design,
        observed.reshape(dense),
        weight_class.reshape(dense),
        calib_unit.reshape(dense),
        class_weight,
        calib_scale.T)],
    )
    row, col = lax.axis_index("rows"), lax.axis_index("grid")
    right_hand = lax.dynamic_slice(extra, (row // 2, 64 * (row % 2) + 8 * col), (1, 8)).reshape(8)
    return gram, right_hand, extra[BLOCKS, 0]


def solution(mesh):
    both = ("rows", "grid")
    return jax.shard_map(
        local,
        mesh=mesh,
        in_specs=(P(both, None), P(both), P(both), P(both), P(), P()),
        out_specs=(P("rows", "grid"), P(both), P()),
        check_vma=False,
    )
```

```python
import functools

import jax
import jax.numpy as jnp
from jax import lax
from jax.experimental import pallas as pl
from jax.experimental.pallas import tpu as pltpu
from jax.sharding import PartitionSpec as P

F32 = jnp.float32
BF16 = jnp.bfloat16
ROWS = 3072
WIDTH = 1024
BLOCKS = 8
LANES = 128
UNITS = 64
CLASSES = 16
LOADS = ((0, 512), (512, 1280), (1792, 1280))
CHUNKS = len(LOADS)
TILE = 64
PARTS = ((0, 24), (24, 16), (40, 24))
RINGS = 3
EXTRA = 16
TOTAL = 393216.0
OFFSETS = (2, 1, 3, 0)
NT = (((1,), (1,)), ((), ()))
MESH = pl.DeviceIdType.MESH


def part_rows(part):
    return pl.ds(*PARTS[part])


def kernel(
    design, observed_in, class_in, unit_in, weight_in, scale_in,
    out, out_extra,
    dbuf, wt, row_scale, row_obs, own, other, arrived, partial,
    ring_x, ring_z, ring_y, first_x, first_z, second_0, second_1, second_2, last_0, last_1, last_2,
    extra_core, extra_ring,
    observed, weight_class, calib_unit, class_weight, scale_t,
    load_sem, small_sem, send_sem, recv_sem,
):
    r = lax.axis_index("rows")
    g = lax.axis_index("grid")
    z, x, y, c = r // 4, r % 4, g // 2, g % 2

    small = [
        pltpu.make_async_copy(src, dst, small_sem.at[i])
        for i, (src, dst) in enumerate([
            (class_in, weight_class), (weight_in, class_weight), (observed_in, observed),
            (unit_in, calib_unit), (scale_in, scale_t),
        ])
    ]
    for copy in small:
        copy.start()
    for q in range(CHUNKS):
        rows = pl.ds(*LOADS[q])
        pltpu.make_async_copy(design.at[rows], dbuf.at[rows], load_sem.at[q]).start()

    def device(dz=0, dx=0, dy=0, flip=False):
        core = 1 - c if flip else c
        return (4 * ((z + dz) % 4) + (x + dx) % 4, 2 * ((y + dy) % 4) + core)

    partner = device(flip=True)
    axis_device = {
        "x": lambda d: device(dx=d),
        "z": lambda d: device(dz=d),
        "y": lambda d: device(dy=d),
    }
    barrier = pltpu.get_barrier_semaphore()
    peers = [partner] + [axis_device[a](d) for a in "xzy" for d in (1, 2, 3)]
    for peer in peers:
        pl.semaphore_signal(barrier, inc=1, device_id=peer, device_id_type=MESH)

    started = []

    def prepare(src, dst, peer):
        index = len(started)
        copy = pltpu.make_async_remote_copy(
            src_ref=src, dst_ref=dst, send_sem=send_sem.at[index],
            recv_sem=recv_sem.at[index], device_id=peer, device_id_type=MESH,
        )
        started.append(copy)
        return copy

    def send(src, dst, peer):
        copy = prepare(src, dst, peer)
        copy.start()
        return copy

    for copy in small:
        copy.wait()
    classes = weight_class[...]
    row_weight = jnp.zeros(classes.shape, F32)
    for k in range(CLASSES):
        row_weight = jnp.where(classes == k, class_weight[k], row_weight)
    root = jnp.sqrt(row_weight)
    obs = observed[...]
    extra_core[c] = jnp.zeros((EXTRA, LANES), F32) + jnp.sum(row_weight * obs * obs)
    root_obs = root * obs
    unit_id = lax.broadcasted_iota(jnp.int32, (UNITS, LANES), 0)
    scales = scale_t[...]
    parts = []
    for _ in range(3):
        parts.append(scales.astype(BF16).astype(F32))
        scales = scales - parts[-1]
    scales = jnp.concatenate(parts, axis=0).astype(BF16)
    obs_line = lax.broadcasted_iota(jnp.int32, (EXTRA, LANES), 0)
    for q in range(ROWS // LANES):
        cols = slice(q * LANES, (q + 1) * LANES)
        hot = jnp.where(unit_id == calib_unit[q : q + 1, :], 1.0, 0.0).astype(BF16)
        triple = jnp.dot(scales, hot, preferred_element_type=F32)
        scale = triple[:BLOCKS] + triple[BLOCKS : 2 * BLOCKS] + triple[2 * BLOCKS :]
        scale = scale * root[q : q + 1, :]
        row_scale[:, cols] = scale
        value = root_obs[q : q + 1, :]
        high = value.astype(BF16).astype(F32)
        both = jnp.where(obs_line == 0, high, jnp.where(obs_line == 1, value - high, 0.0))
        row_obs[:, cols] = both.astype(BF16)

    def block_at(position):
        core = c if position % 2 else 1 - c
        return (y + OFFSETS[position // 2]) % 4, core

    def weigh(q):
        rows = pl.ds(*LOADS[q])
        pltpu.make_async_copy(design.at[rows], dbuf.at[rows], load_sem.at[q]).wait()
        for position in range(BLOCKS):
            high, core = block_at(position)
            block = 2 * high + core
            cols = pl.ds(pl.multiple_of(block * LANES, LANES), LANES)
            piece = dbuf[rows, cols].T.astype(F32)
            wt[position, :, rows] = (piece * row_scale[pl.ds(block, 1), rows]).astype(BF16)

    def store(row_position, col_position, value):
        target = own if col_position % 2 else other
        high, core = block_at(row_position)
        for half in range(2):
            target[col_position // 2, high, 2 * core + half] = value[64 * half : 64 * half + 64]

    squares = [(i, j) for j in range(4) for i in range(j, 4)]

    def multiply(i, j, step):
        start, count = LOADS[step]
        cols = slice(start, start + count)
        left = wt[2 * i : 2 * i + 2, :, cols].reshape(2 * LANES, count)
        if i == j:
            left = jnp.concatenate([left, row_obs[:, cols]], axis=0)
        right = wt[2 * j : 2 * j + 2, :, cols].reshape(2 * LANES, count)
        product = lax.dot_general(left, right, NT, preferred_element_type=F32)
        place, lines = squares.index((i, j)), product.shape[0]
        if step:
            product = product + partial[place, :lines]
        if step + 1 < CHUNKS:
            partial[place, :lines] = product
        else:
            keep(i, j, product)

    def keep(i, j, product):
        for a in range(2):
            for b in range(2):
                value = product[a * LANES : (a + 1) * LANES, b * LANES : (b + 1) * LANES]
                store(2 * i + a, 2 * j + b, value)
                if i > j:
                    store(2 * j + b, 2 * i + a, value.T)
        if i == j:
            line = 2 * LANES
            rhs = product[line : line + 1] + product[line + 1 : line + 2]
            for b in range(2):
                high, core = block_at(2 * j + b)
                extra_core[c, pl.ds(2 * high + core, 1), :] = rhs[:, b * LANES : (b + 1) * LANES]

    def panel(k, step=CHUNKS - 1):
        for i in range(k, 4):
            multiply(i, k, step)

    exchanged = {}

    def exchange(j):
        pairs = [(j, i) for i in range(j, 4)] + [(i, j) for i in range(j + 1, 4)]
        for k, i in pairs:
            line = (y + OFFSETS[i]) % 4
            exchanged[k, i] = send(other.at[k, line], arrived.at[k, line], partner)

    def merge(k):
        for i in range(4):
            exchanged[k, i].wait_recv()

        def add(i, _):
            own[k, i] = own[k, i] + arrived[k, i]
            return 0

        lax.fori_loop(0, 4, add, 0)

    def scatter(axis, src, bufs):
        to = axis_device[axis]
        return [(prepare(src(d), bufs.at[d - 1], to(d)), bufs.at[d - 1]) for d in (2, 1, 3)]

    def start(copies):
        for copy, _ in copies:
            copy.start()
        return copies

    def gather(src, copies):
        for copy, _ in copies:
            copy.wait_recv()
        mine = src(0)
        total = mine[...]
        for _, buf in copies:
            total = total + buf[...]
        mine[...] = total

    class Ring:
        def __init__(self, axis, src, bufs):
            right, left = axis_device[axis](1), axis_device[axis](3)
            self.src, self.bufs = src, bufs
            self.hop_a = prepare(src(2, 0), bufs.at[0], right)
            self.hop_b = prepare(src(2, 1), bufs.at[1], left)
            self.direct_b = prepare(src(1, 1), bufs.at[3], right)
            self.direct_a = prepare(src(3, 0), bufs.at[2], left)
            self.last_a = prepare(bufs.at[0], bufs.at[4], right)
            self.last_b = prepare(bufs.at[1], bufs.at[5], left)
            self.next_a, self.next_b = src(1, 0), src(3, 1)

        def start_far(self):
            self.hop_a.start()
            self.hop_b.start()

        def start_right(self):
            self.direct_b.start()

        def start_left(self):
            self.direct_a.start()

        def start(self):
            self.start_far()
            self.start_right()
            self.start_left()

        def pass_right(self):
            self.hop_a.wait_recv()
            self.bufs[0] = self.bufs[0] + self.next_a[...]
            self.last_a.start()

        def pass_left(self):
            self.hop_b.wait_recv()
            self.bufs[1] = self.bufs[1] + self.next_b[...]
            self.last_b.start()

        def finish(self):
            for half, direct, via in ((0, self.direct_a, self.last_a), (1, self.direct_b, self.last_b)):
                direct.wait_recv()
                via.wait_recv()
                mine = self.src(0, half)
                mine[...] = mine[...] + self.bufs[2 + half] + self.bufs[4 + half]

    panel_of = {2: 0, 1: 1, 3: 2, 0: 3}

    def at(part, k, dz, dx):
        return own.at[k, dz, dx, part_rows(part), :]

    every = slice(None)

    def two(half):
        return pl.ds(2 * half, 2)

    def half_x(k):
        return lambda d, half: at(0, k, two(half), (x + d) % 4)

    def half_z(k):
        return lambda d, half: at(2, k, (z + d) % 4, two(half))

    def half_y(d, half):
        return at(1, panel_of[d], two(half), every)

    def src_x(k):
        return lambda d: at(0, k, every, (x + d) % 4)

    def src_z(k):
        return lambda d: at(2, k, (z + d) % 4, every)

    def src_0y(d):
        return at(0, panel_of[d], every, x)

    def src_1z(d):
        return at(1, 3, (z + d) % 4, every)

    def src_2x(k):
        return lambda d: at(2, k, z, (x + d) % 4)

    def src_0z(d):
        return at(0, 3, (z + d) % 4, x)

    def src_1x(d):
        return at(1, 3, z, (x + d) % 4)

    def src_2y(d):
        return at(2, panel_of[d], z, x)

    to_y = axis_device["y"]
    distance_of = (2, 1, 3, 0)
    step_0y, step_2x, step_2y = [], {}, []
    rings = {k: (Ring("x", half_x(k), ring_x.at[k]), Ring("z", half_z(k), ring_z.at[k])) for k in range(RINGS)}
    ring_of_y = Ring("y", half_y, ring_y)

    step_x = {k: scatter("x", src_x(k), first_x.at[k - RINGS]) for k in range(RINGS, 4)}
    step_z = {k: scatter("z", src_z(k), first_z.at[k - RINGS]) for k in range(RINGS, 4)}

    def spread(k):
        if k < RINGS:
            for ring in rings[k]:
                ring.start()
        else:
            start(step_x[k])
            start(step_z[k])
        if k == 0:
            ring_of_y.start_far()
        if k == 1:
            ring_of_y.start_right()
        if k == 2:
            ring_of_y.start_left()

    def pass_on(k):
        for ring in rings[k]:
            ring.pass_right()
            ring.pass_left()

    def finish_x(k):
        if k < RINGS:
            rings[k][0].finish()
        else:
            gather(src_x(k), step_x[k])

    def finish_z(k):
        if k < RINGS:
            rings[k][1].finish()
        else:
            gather(src_z(k), step_z[k])

    def gather_extra(stage, copies):
        for copy in copies:
            copy.wait_recv()
        total = extra_ring[stage, 0] + extra_ring[stage, 1]
        return total + extra_ring[stage, 2] + extra_ring[stage, 3]

    def spread_extra(stage, total):
        place = (x, y, z)[stage]
        to = axis_device["xyz"[stage]]
        extra_ring[stage, place] = total
        slot = extra_ring.at[stage, place]
        return [send(slot, slot, to(d)) for d in (2, 1, 3)]

    weigh(0)
    for step in range(1, CHUNKS):
        weigh(step)
        for k in range(4):
            panel(k, step - 1)
    panel(0)
    pl.semaphore_wait(barrier, len(peers))
    exchange(0)
    panel(1)
    exchange(1)
    panel(2)
    exchange(2)
    panel(3)
    exchange(3)
    slot = extra_core.at[c]
    sent_extra = send(slot, slot, partner)
    merge(0)
    spread(0)
    merge(1)
    spread(1)
    merge(2)
    spread(2)
    pass_on(0)
    merge(3)
    spread(3)
    ring_of_y.pass_right()
    ring_of_y.pass_left()
    for k in range(1, RINGS):
        pass_on(k)
    sent_extra.wait_recv()
    extra = spread_extra(0, extra_core[0] + extra_core[1])
    for k in range(4):
        finish_x(k)
        if k < 3:
            d = distance_of[k]
            step_0y.append((send(src_0y(d), second_0.at[k], to_y(d)), second_0.at[k]))
        finish_z(k)
        step_2x[k] = start(scatter("x", src_2x(k), second_2.at[k]))
    extra = spread_extra(1, gather_extra(0, extra))
    ring_of_y.finish()
    step_1z = start(scatter("z", src_1z, second_1))
    gather(src_0y, step_0y)
    step_0z = start(scatter("z", src_0z, last_0))
    for k in range(4):
        gather(src_2x(k), step_2x[k])
        if k < 3:
            d = distance_of[k]
            step_2y.append((send(src_2y(d), last_2.at[k], to_y(d)), last_2.at[k]))
    extra = spread_extra(2, gather_extra(1, extra))
    gather(src_1z, step_1z)
    step_1x = start(scatter("x", src_1x, last_1))
    for part, src, copies in ((0, src_0z, step_0z), (2, src_2y, step_2y), (1, src_1x, step_1x)):
        for copy, _ in copies:
            copy.wait_recv()
        total = src(0)[...]
        for _, buf in copies:
            total = total + buf[...]
        out[part_rows(part), :] = total * (1.0 / TOTAL)
    out_extra[...] = gather_extra(2, extra) * (1.0 / TOTAL)
    for copy in started:
        copy.wait_send()


def split(gram, extra, out_gram, out_rhs, out_chi):
    r, g = lax.axis_index("rows"), lax.axis_index("grid")
    out_gram[...] = gram[...]
    line = extra[pl.ds(r // 2, 1), :]
    line = pltpu.roll(line, (2 * LANES - (64 * (r % 2) + 8 * g)) % LANES, 1)
    out_rhs[...] = line[0, :8]
    out_chi[0] = extra[BLOCKS, 0]


COPIES = 16 + 2 * (6 * RINGS + 3 * (4 - RINGS)) + 6 + 3 + 3 + 12 + 9 + 10


def local(design, observed, weight_class, calib_unit, class_weight, calib_scale):
    dense = (ROWS // LANES, LANES)
    vmem = pl.BlockSpec(memory_space=pltpu.VMEM)
    panels = pltpu.VMEM((4, 4, 4, TILE, LANES), F32)
    rows_x, rows_y, rows_z = (rows for _, rows in PARTS)
    gram, extra = pl.pallas_call(
        kernel,
        out_shape=(jax.ShapeDtypeStruct((TILE, LANES), F32), jax.ShapeDtypeStruct((EXTRA, LANES), F32)),
        in_specs=[pl.BlockSpec(memory_space=pltpu.HBM)] * 6,
        out_specs=(vmem, vmem),
        scratch_shapes=[
            pltpu.VMEM((ROWS, WIDTH), BF16),
            pltpu.VMEM((BLOCKS, LANES, ROWS), BF16),
            pltpu.VMEM((BLOCKS, ROWS), F32),
            pltpu.VMEM((EXTRA, ROWS), BF16),
            panels, panels, panels,
            pltpu.VMEM((10, 2 * LANES + EXTRA, 2 * LANES), F32),
            pltpu.VMEM((RINGS, 6, 2, rows_x, LANES), F32),
            pltpu.VMEM((RINGS, 6, 2, rows_z, LANES), F32),
            pltpu.VMEM((6, 2, 4, rows_y, LANES), F32),
            pltpu.VMEM((4 - RINGS, 3, 4, rows_x, LANES), F32),
            pltpu.VMEM((4 - RINGS, 3, 4, rows_z, LANES), F32),
            pltpu.VMEM((3, 4, rows_x, LANES), F32),
            pltpu.VMEM((3, 4, rows_y, LANES), F32),
            pltpu.VMEM((4, 3, rows_z, LANES), F32),
            pltpu.VMEM((3, rows_x, LANES), F32),
            pltpu.VMEM((3, rows_y, LANES), F32),
            pltpu.VMEM((3, rows_z, LANES), F32),
            pltpu.VMEM((2, EXTRA, LANES), F32),
            pltpu.VMEM((3, 4, EXTRA, LANES), F32),
            pltpu.VMEM(dense, F32),
            pltpu.VMEM(dense, jnp.int32),
            pltpu.VMEM(dense, jnp.int32),
            pltpu.SMEM((CLASSES,), F32),
            pltpu.VMEM((BLOCKS, UNITS), F32),
            pltpu.SemaphoreType.DMA((CHUNKS,)),
            pltpu.SemaphoreType.DMA((5,)),
            pltpu.SemaphoreType.DMA((COPIES,)),
            pltpu.SemaphoreType.DMA((COPIES,)),
        ],
        compiler_params=pltpu.CompilerParams(
            collective_id=0, has_side_effects=True, vmem_limit_bytes=32 * 2**20
        ),
    )(
        *[pltpu.with_memory_space_constraint(v, pltpu.HBM) for v in (design,
        observed.reshape(dense),
        weight_class.reshape(dense),
        calib_unit.reshape(dense),
        class_weight,
        calib_scale.T)],
    )
    gram, right_hand, chi = pl.pallas_call(
        split,
        out_shape=(
            jax.ShapeDtypeStruct((TILE, LANES), F32),
            jax.ShapeDtypeStruct((8,), F32),
            jax.ShapeDtypeStruct((1,), F32),
        ),
        in_specs=[vmem, vmem],
        out_specs=(vmem, vmem, pl.BlockSpec(memory_space=pltpu.SMEM)),
        compiler_params=pltpu.CompilerParams(vmem_limit_bytes=2**20),
    )(gram, extra)
    return gram, right_hand, chi.reshape(())


def solution(mesh):
    both = ("rows", "grid")
    return jax.shard_map(
        local,
        mesh=mesh,
        in_specs=(P(both, None), P(both), P(both), P(both), P(), P()),
        out_specs=(P("rows", "grid"), P(both), P()),
        check_vma=False,
    )
```

```python
import functools

import jax
import jax.numpy as jnp
from jax import lax
from jax.experimental import pallas as pl
from jax.experimental.pallas import tpu as pltpu
from jax.sharding import PartitionSpec as P

F32 = jnp.float32
BF16 = jnp.bfloat16
ROWS = 3072
WIDTH = 1024
BLOCKS = 8
LANES = 128
UNITS = 64
CLASSES = 16
LOADS = ((0, 512), (512, 1280), (1792, 1280))
CHUNKS = len(LOADS)
TILE = 64
PARTS = ((0, 24), (24, 16), (40, 24))
RINGS = 3
EXTRA = 16
TOTAL = 393216.0
OFFSETS = (2, 1, 3, 0)
NT = (((1,), (1,)), ((), ()))
MESH = pl.DeviceIdType.MESH


def part_rows(part):
    return pl.ds(*PARTS[part])


def kernel(
    design, observed_in, class_in, unit_in, weight_in, scale_in,
    out, out_extra,
    dbuf, wt, row_scale, row_obs, own, other, arrived, partial,
    ring_x, ring_z, ring_y, first_x, first_z, second_0, second_1, second_2, last_0, last_1, last_2,
    extra_core, extra_ring,
    observed, weight_class, calib_unit, class_weight, scale_t,
    load_sem, small_sem, send_sem, recv_sem,
):
    r = lax.axis_index("rows")
    g = lax.axis_index("grid")
    z, x, y, c = r // 4, r % 4, g // 2, g % 2

    small = [
        pltpu.make_async_copy(src, dst, small_sem.at[i])
        for i, (src, dst) in enumerate([
            (class_in, weight_class), (weight_in, class_weight), (observed_in, observed),
            (unit_in, calib_unit), (scale_in, scale_t),
        ])
    ]
    for copy in small:
        copy.start()
    for q in range(CHUNKS):
        rows = pl.ds(*LOADS[q])
        pltpu.make_async_copy(design.at[rows], dbuf.at[rows], load_sem.at[q]).start()

    def device(dz=0, dx=0, dy=0, flip=False):
        core = 1 - c if flip else c
        return (4 * ((z + dz) % 4) + (x + dx) % 4, 2 * ((y + dy) % 4) + core)

    partner = device(flip=True)
    axis_device = {
        "x": lambda d: device(dx=d),
        "z": lambda d: device(dz=d),
        "y": lambda d: device(dy=d),
    }
    barrier = pltpu.get_barrier_semaphore()
    peers = [partner] + [axis_device[a](d) for a in "xzy" for d in (1, 2, 3)]
    for peer in peers:
        pl.semaphore_signal(barrier, inc=1, device_id=peer, device_id_type=MESH)

    started = []

    def prepare(src, dst, peer):
        index = len(started)
        copy = pltpu.make_async_remote_copy(
            src_ref=src, dst_ref=dst, send_sem=send_sem.at[index],
            recv_sem=recv_sem.at[index], device_id=peer, device_id_type=MESH,
        )
        started.append(copy)
        return copy

    def send(src, dst, peer):
        copy = prepare(src, dst, peer)
        copy.start()
        return copy

    for copy in small:
        copy.wait()
    classes = weight_class[...]
    row_weight = jnp.zeros(classes.shape, F32)
    for k in range(CLASSES):
        row_weight = jnp.where(classes == k, class_weight[k], row_weight)
    root = jnp.sqrt(row_weight)
    obs = observed[...]
    extra_core[c] = jnp.zeros((EXTRA, LANES), F32) + jnp.sum(row_weight * obs * obs)
    root_obs = root * obs
    unit_id = lax.broadcasted_iota(jnp.int32, (UNITS, LANES), 0)
    scales = scale_t[...]
    parts = []
    for _ in range(3):
        parts.append(scales.astype(BF16).astype(F32))
        scales = scales - parts[-1]
    scales = jnp.concatenate(parts, axis=0).astype(BF16)
    obs_line = lax.broadcasted_iota(jnp.int32, (EXTRA, LANES), 0)
    for q in range(ROWS // LANES):
        cols = slice(q * LANES, (q + 1) * LANES)
        hot = jnp.where(unit_id == calib_unit[q : q + 1, :], 1.0, 0.0).astype(BF16)
        triple = jnp.dot(scales, hot, preferred_element_type=F32)
        scale = triple[:BLOCKS] + triple[BLOCKS : 2 * BLOCKS] + triple[2 * BLOCKS :]
        scale = scale * root[q : q + 1, :]
        row_scale[:, cols] = scale
        value = root_obs[q : q + 1, :]
        high = value.astype(BF16).astype(F32)
        both = jnp.where(obs_line == 0, high, jnp.where(obs_line == 1, value - high, 0.0))
        row_obs[:, cols] = both.astype(BF16)

    def block_at(position):
        core = c if position % 2 else 1 - c
        return (y + OFFSETS[position // 2]) % 4, core

    def weigh(q):
        rows = pl.ds(*LOADS[q])
        pltpu.make_async_copy(design.at[rows], dbuf.at[rows], load_sem.at[q]).wait()
        for position in range(BLOCKS):
            high, core = block_at(position)
            block = 2 * high + core
            cols = pl.ds(pl.multiple_of(block * LANES, LANES), LANES)
            piece = dbuf[rows, cols].T.astype(F32)
            wt[position, :, rows] = (piece * row_scale[pl.ds(block, 1), rows]).astype(BF16)

    def store(row_position, col_position, value):
        target = own if col_position % 2 else other
        high, core = block_at(row_position)
        for half in range(2):
            target[col_position // 2, high, 2 * core + half] = value[64 * half : 64 * half + 64]

    squares = [(i, j) for j in range(4) for i in range(j, 4)]

    def multiply(i, j, step):
        start, count = LOADS[step]
        cols = slice(start, start + count)
        left = wt[2 * i : 2 * i + 2, :, cols].reshape(2 * LANES, count)
        if i == j:
            left = jnp.concatenate([left, row_obs[:, cols]], axis=0)
        right = wt[2 * j : 2 * j + 2, :, cols].reshape(2 * LANES, count)
        product = lax.dot_general(left, right, NT, preferred_element_type=F32)
        place, lines = squares.index((i, j)), product.shape[0]
        if step:
            product = product + partial[place, :lines]
        if step + 1 < CHUNKS:
            partial[place, :lines] = product
        else:
            keep(i, j, product)

    def keep(i, j, product):
        for a in range(2):
            for b in range(2):
                value = product[a * LANES : (a + 1) * LANES, b * LANES : (b + 1) * LANES]
                store(2 * i + a, 2 * j + b, value)
                if i > j:
                    store(2 * j + b, 2 * i + a, value.T)
        if i == j:
            line = 2 * LANES
            rhs = product[line : line + 1] + product[line + 1 : line + 2]
            for b in range(2):
                high, core = block_at(2 * j + b)
                extra_core[c, pl.ds(2 * high + core, 1), :] = rhs[:, b * LANES : (b + 1) * LANES]

    def panel(k, step=CHUNKS - 1):
        for i in range(k, 4):
            multiply(i, k, step)

    exchanged = {}

    def exchange(j):
        pairs = [(j, i) for i in range(j, 4)] + [(i, j) for i in range(j + 1, 4)]
        for k, i in pairs:
            line = (y + OFFSETS[i]) % 4
            exchanged[k, i] = send(other.at[k, line], arrived.at[k, line], partner)

    def merge(k):
        for i in range(4):
            exchanged[k, i].wait_recv()

        def add(i, _):
            own[k, i] = own[k, i] + arrived[k, i]
            return 0

        lax.fori_loop(0, 4, add, 0)

    def scatter(axis, src, bufs):
        to = axis_device[axis]
        return [(prepare(src(d), bufs.at[d - 1], to(d)), bufs.at[d - 1]) for d in (2, 1, 3)]

    def start(copies):
        for copy, _ in copies:
            copy.start()
        return copies

    def gather(src, copies):
        for copy, _ in copies:
            copy.wait_recv()
        mine = src(0)
        total = mine[...]
        for _, buf in copies:
            total = total + buf[...]
        mine[...] = total

    class Ring:
        def __init__(self, axis, src, bufs):
            right, left = axis_device[axis](1), axis_device[axis](3)
            self.src, self.bufs = src, bufs
            self.hop_a = prepare(src(2, 0), bufs.at[0], right)
            self.hop_b = prepare(src(2, 1), bufs.at[1], left)
            self.direct_b = prepare(src(1, 1), bufs.at[3], right)
            self.direct_a = prepare(src(3, 0), bufs.at[2], left)
            self.last_a = prepare(bufs.at[0], bufs.at[4], right)
            self.last_b = prepare(bufs.at[1], bufs.at[5], left)
            self.next_a, self.next_b = src(1, 0), src(3, 1)

        def start_far(self):
            self.hop_a.start()
            self.hop_b.start()

        def start_right(self):
            self.direct_b.start()

        def start_left(self):
            self.direct_a.start()

        def start(self):
            self.start_far()
            self.start_right()
            self.start_left()

        def pass_right(self):
            self.hop_a.wait_recv()
            self.bufs[0] = self.bufs[0] + self.next_a[...]
            self.last_a.start()

        def pass_left(self):
            self.hop_b.wait_recv()
            self.bufs[1] = self.bufs[1] + self.next_b[...]
            self.last_b.start()

        def finish(self):
            for half, direct, via in ((0, self.direct_a, self.last_a), (1, self.direct_b, self.last_b)):
                direct.wait_recv()
                via.wait_recv()
                mine = self.src(0, half)
                mine[...] = mine[...] + self.bufs[2 + half] + self.bufs[4 + half]

    panel_of = {2: 0, 1: 1, 3: 2, 0: 3}

    def at(part, k, dz, dx):
        return own.at[k, dz, dx, part_rows(part), :]

    every = slice(None)

    def two(half):
        return pl.ds(2 * half, 2)

    def half_x(k):
        return lambda d, half: at(0, k, two(half), (x + d) % 4)

    def half_z(k):
        return lambda d, half: at(2, k, (z + d) % 4, two(half))

    def half_y(d, half):
        return at(1, panel_of[d], two(half), every)

    def src_x(k):
        return lambda d: at(0, k, every, (x + d) % 4)

    def src_z(k):
        return lambda d: at(2, k, (z + d) % 4, every)

    def src_0y(d):
        return at(0, panel_of[d], every, x)

    def src_1z(d):
        return at(1, 3, (z + d) % 4, every)

    def src_2x(k):
        return lambda d: at(2, k, z, (x + d) % 4)

    def src_0z(d):
        return at(0, 3, (z + d) % 4, x)

    def src_1x(d):
        return at(1, 3, z, (x + d) % 4)

    def src_2y(d):
        return at(2, panel_of[d], z, x)

    to_y = axis_device["y"]
    distance_of = (2, 1, 3, 0)
    step_0y, step_2x, step_2y = [], {}, []
    rings = {k: (Ring("x", half_x(k), ring_x.at[k]), Ring("z", half_z(k), ring_z.at[k])) for k in range(RINGS)}
    ring_of_y = Ring("y", half_y, ring_y)

    step_x = {k: scatter("x", src_x(k), first_x.at[k - RINGS]) for k in range(RINGS, 4)}
    step_z = {k: scatter("z", src_z(k), first_z.at[k - RINGS]) for k in range(RINGS, 4)}

    def spread(k):
        if k < RINGS:
            for ring in rings[k]:
                ring.start()
        else:
            start(step_x[k])
            start(step_z[k])
        if k == 0:
            ring_of_y.start_far()
        if k == 1:
            ring_of_y.start_right()
        if k == 2:
            ring_of_y.start_left()

    def pass_on(k):
        for ring in rings[k]:
            ring.pass_right()
            ring.pass_left()

    def finish_x(k):
        if k < RINGS:
            rings[k][0].finish()
        else:
            gather(src_x(k), step_x[k])

    def finish_z(k):
        if k < RINGS:
            rings[k][1].finish()
        else:
            gather(src_z(k), step_z[k])

    def gather_extra(stage, copies):
        for copy in copies:
            copy.wait_recv()
        total = extra_ring[stage, 0] + extra_ring[stage, 1]
        return total + extra_ring[stage, 2] + extra_ring[stage, 3]

    def spread_extra(stage, total):
        place = (x, y, z)[stage]
        to = axis_device["xyz"[stage]]
        extra_ring[stage, place] = total
        slot = extra_ring.at[stage, place]
        return [send(slot, slot, to(d)) for d in (2, 1, 3)]

    weigh(0)
    for step in range(1, CHUNKS):
        weigh(step)
        for k in range(4):
            panel(k, step - 1)
    panel(0)
    pl.semaphore_wait(barrier, len(peers))
    exchange(0)
    panel(1)
    exchange(1)
    panel(2)
    exchange(2)
    panel(3)
    exchange(3)
    slot = extra_core.at[c]
    sent_extra = send(slot, slot, partner)
    merge(0)
    spread(0)
    merge(1)
    spread(1)
    merge(2)
    spread(2)
    pass_on(0)
    merge(3)
    spread(3)
    ring_of_y.pass_right()
    ring_of_y.pass_left()
    for k in range(1, RINGS):
        pass_on(k)
    sent_extra.wait_recv()
    extra = spread_extra(0, extra_core[0] + extra_core[1])
    def finish(k):
        finish_x(k)
        if k < 3:
            d = distance_of[k]
            step_0y.append((send(src_0y(d), second_0.at[k], to_y(d)), second_0.at[k]))
        finish_z(k)
        step_2x[k] = start(scatter("x", src_2x(k), second_2.at[k]))

    finish(0)
    finish(1)
    ring_of_y.finish()
    step_1z = start(scatter("z", src_1z, second_1))
    finish(2)
    finish(3)
    extra = spread_extra(1, gather_extra(0, extra))
    gather(src_0y, step_0y)
    step_0z = start(scatter("z", src_0z, last_0))
    for k in range(4):
        gather(src_2x(k), step_2x[k])
        if k < 3:
            d = distance_of[k]
            step_2y.append((send(src_2y(d), last_2.at[k], to_y(d)), last_2.at[k]))
    extra = spread_extra(2, gather_extra(1, extra))
    gather(src_1z, step_1z)
    step_1x = start(scatter("x", src_1x, last_1))
    for part, src, copies in ((0, src_0z, step_0z), (2, src_2y, step_2y), (1, src_1x, step_1x)):
        for copy, _ in copies:
            copy.wait_recv()
        total = src(0)[...]
        for _, buf in copies:
            total = total + buf[...]
        out[part_rows(part), :] = total * (1.0 / TOTAL)
    out_extra[...] = gather_extra(2, extra) * (1.0 / TOTAL)
    for copy in started:
        copy.wait_send()


def split(gram, extra, out_gram, out_rhs, out_chi):
    r, g = lax.axis_index("rows"), lax.axis_index("grid")
    out_gram[...] = gram[...]
    line = extra[pl.ds(r // 2, 1), :]
    line = pltpu.roll(line, (2 * LANES - (64 * (r % 2) + 8 * g)) % LANES, 1)
    out_rhs[...] = line[0, :8]
    out_chi[0] = extra[BLOCKS, 0]


COPIES = 16 + 2 * (6 * RINGS + 3 * (4 - RINGS)) + 6 + 3 + 3 + 12 + 9 + 10


def local(design, observed, weight_class, calib_unit, class_weight, calib_scale):
    dense = (ROWS // LANES, LANES)
    vmem = pl.BlockSpec(memory_space=pltpu.VMEM)
    panels = pltpu.VMEM((4, 4, 4, TILE, LANES), F32)
    rows_x, rows_y, rows_z = (rows for _, rows in PARTS)
    gram, extra = pl.pallas_call(
        kernel,
        out_shape=(jax.ShapeDtypeStruct((TILE, LANES), F32), jax.ShapeDtypeStruct((EXTRA, LANES), F32)),
        in_specs=[pl.BlockSpec(memory_space=pltpu.HBM)] * 6,
        out_specs=(vmem, vmem),
        scratch_shapes=[
            pltpu.VMEM((ROWS, WIDTH), BF16),
            pltpu.VMEM((BLOCKS, LANES, ROWS), BF16),
            pltpu.VMEM((BLOCKS, ROWS), F32),
            pltpu.VMEM((EXTRA, ROWS), BF16),
            panels, panels, panels,
            pltpu.VMEM((10, 2 * LANES + EXTRA, 2 * LANES), F32),
            pltpu.VMEM((RINGS, 6, 2, rows_x, LANES), F32),
            pltpu.VMEM((RINGS, 6, 2, rows_z, LANES), F32),
            pltpu.VMEM((6, 2, 4, rows_y, LANES), F32),
            pltpu.VMEM((4 - RINGS, 3, 4, rows_x, LANES), F32),
            pltpu.VMEM((4 - RINGS, 3, 4, rows_z, LANES), F32),
            pltpu.VMEM((3, 4, rows_x, LANES), F32),
            pltpu.VMEM((3, 4, rows_y, LANES), F32),
            pltpu.VMEM((4, 3, rows_z, LANES), F32),
            pltpu.VMEM((3, rows_x, LANES), F32),
            pltpu.VMEM((3, rows_y, LANES), F32),
            pltpu.VMEM((3, rows_z, LANES), F32),
            pltpu.VMEM((2, EXTRA, LANES), F32),
            pltpu.VMEM((3, 4, EXTRA, LANES), F32),
            pltpu.VMEM(dense, F32),
            pltpu.VMEM(dense, jnp.int32),
            pltpu.VMEM(dense, jnp.int32),
            pltpu.SMEM((CLASSES,), F32),
            pltpu.VMEM((BLOCKS, UNITS), F32),
            pltpu.SemaphoreType.DMA((CHUNKS,)),
            pltpu.SemaphoreType.DMA((5,)),
            pltpu.SemaphoreType.DMA((COPIES,)),
            pltpu.SemaphoreType.DMA((COPIES,)),
        ],
        compiler_params=pltpu.CompilerParams(
            collective_id=0, has_side_effects=True, vmem_limit_bytes=32 * 2**20
        ),
    )(
        *[pltpu.with_memory_space_constraint(v, pltpu.HBM) for v in (design,
        observed.reshape(dense),
        weight_class.reshape(dense),
        calib_unit.reshape(dense),
        class_weight,
        calib_scale.T)],
    )
    gram, right_hand, chi = pl.pallas_call(
        split,
        out_shape=(
            jax.ShapeDtypeStruct((TILE, LANES), F32),
            jax.ShapeDtypeStruct((8,), F32),
            jax.ShapeDtypeStruct((1,), F32),
        ),
        in_specs=[vmem, vmem],
        out_specs=(vmem, vmem, pl.BlockSpec(memory_space=pltpu.SMEM)),
        compiler_params=pltpu.CompilerParams(vmem_limit_bytes=2**20),
    )(gram, extra)
    return gram, right_hand, chi.reshape(())


def solution(mesh):
    both = ("rows", "grid")
    return jax.shard_map(
        local,
        mesh=mesh,
        in_specs=(P(both, None), P(both), P(both), P(both), P(), P()),
        out_specs=(P("rows", "grid"), P(both), P()),
        check_vma=False,
    )
```

```python
import functools

import jax
import jax.numpy as jnp
from jax import lax
from jax.experimental import pallas as pl
from jax.experimental.pallas import tpu as pltpu
from jax.sharding import PartitionSpec as P

F32 = jnp.float32
BF16 = jnp.bfloat16
ROWS = 3072
WIDTH = 1024
BLOCKS = 8
LANES = 128
UNITS = 64
CLASSES = 16
LOADS = ((0, 512), (512, 1280), (1792, 1280))
CHUNKS = len(LOADS)
TILE = 64
PARTS = ((0, 24), (24, 16), (40, 24))
RINGS = 3
EXTRA = 16
TOTAL = 393216.0
OFFSETS = (2, 1, 3, 0)
NT = (((1,), (1,)), ((), ()))
MESH = pl.DeviceIdType.MESH


def part_rows(part):
    return pl.ds(*PARTS[part])


def kernel(
    design, observed_in, class_in, unit_in, weight_in, scale_in,
    out, out_extra,
    dbuf, wt, row_scale, row_obs, own, other, arrived, partial,
    ring_x, ring_z, ring_y, first_x, first_z, second_0, second_1, second_2, last_0, last_1, last_2,
    extra_core, extra_ring,
    observed, weight_class, calib_unit, class_weight, scale_t,
    load_sem, small_sem, send_sem, recv_sem,
):
    r = lax.axis_index("rows")
    g = lax.axis_index("grid")
    z, x, y, c = r // 4, r % 4, g // 2, g % 2

    small = [
        pltpu.make_async_copy(src, dst, small_sem.at[i])
        for i, (src, dst) in enumerate([
            (class_in, weight_class), (weight_in, class_weight), (observed_in, observed),
            (unit_in, calib_unit), (scale_in, scale_t),
        ])
    ]
    for copy in small:
        copy.start()
    for q in range(CHUNKS):
        rows = pl.ds(*LOADS[q])
        pltpu.make_async_copy(design.at[rows], dbuf.at[rows], load_sem.at[q]).start()

    def device(dz=0, dx=0, dy=0, flip=False):
        core = 1 - c if flip else c
        return (4 * ((z + dz) % 4) + (x + dx) % 4, 2 * ((y + dy) % 4) + core)

    partner = device(flip=True)
    axis_device = {
        "x": lambda d: device(dx=d),
        "z": lambda d: device(dz=d),
        "y": lambda d: device(dy=d),
    }
    barrier = pltpu.get_barrier_semaphore()
    peers = [partner] + [axis_device[a](d) for a in "xzy" for d in (1, 2, 3)]
    for peer in peers:
        pl.semaphore_signal(barrier, inc=1, device_id=peer, device_id_type=MESH)

    started = []

    def prepare(src, dst, peer):
        index = len(started)
        copy = pltpu.make_async_remote_copy(
            src_ref=src, dst_ref=dst, send_sem=send_sem.at[index],
            recv_sem=recv_sem.at[index], device_id=peer, device_id_type=MESH,
        )
        started.append(copy)
        return copy

    def send(src, dst, peer):
        copy = prepare(src, dst, peer)
        copy.start()
        return copy

    for copy in small:
        copy.wait()
    classes = weight_class[...]
    row_weight = jnp.zeros(classes.shape, F32)
    for k in range(CLASSES):
        row_weight = jnp.where(classes == k, class_weight[k], row_weight)
    root = jnp.sqrt(row_weight)
    obs = observed[...]
    extra_core[c] = jnp.zeros((EXTRA, LANES), F32) + jnp.sum(row_weight * obs * obs)
    root_obs = root * obs
    unit_id = lax.broadcasted_iota(jnp.int32, (UNITS, LANES), 0)
    scales = scale_t[...]
    parts = []
    for _ in range(3):
        parts.append(scales.astype(BF16).astype(F32))
        scales = scales - parts[-1]
    scales = jnp.concatenate(parts, axis=0).astype(BF16)
    obs_line = lax.broadcasted_iota(jnp.int32, (EXTRA, LANES), 0)
    for q in range(ROWS // LANES):
        cols = slice(q * LANES, (q + 1) * LANES)
        hot = jnp.where(unit_id == calib_unit[q : q + 1, :], 1.0, 0.0).astype(BF16)
        triple = jnp.dot(scales, hot, preferred_element_type=F32)
        scale = triple[:BLOCKS] + triple[BLOCKS : 2 * BLOCKS] + triple[2 * BLOCKS :]
        scale = scale * root[q : q + 1, :]
        row_scale[:, cols] = scale
        value = root_obs[q : q + 1, :]
        high = value.astype(BF16).astype(F32)
        both = jnp.where(obs_line == 0, high, jnp.where(obs_line == 1, value - high, 0.0))
        row_obs[:, cols] = both.astype(BF16)

    def block_at(position):
        core = c if position % 2 else 1 - c
        return (y + OFFSETS[position // 2]) % 4, core

    def weigh(q):
        rows = pl.ds(*LOADS[q])
        pltpu.make_async_copy(design.at[rows], dbuf.at[rows], load_sem.at[q]).wait()
        for position in range(BLOCKS):
            high, core = block_at(position)
            block = 2 * high + core
            cols = pl.ds(pl.multiple_of(block * LANES, LANES), LANES)
            piece = dbuf[rows, cols].T.astype(F32)
            wt[position, :, rows] = (piece * row_scale[pl.ds(block, 1), rows]).astype(BF16)

    def store(row_position, col_position, value):
        target = own if col_position % 2 else other
        high, core = block_at(row_position)
        for half in range(2):
            target[col_position // 2, high, 2 * core + half] = value[64 * half : 64 * half + 64]

    squares = [(i, j) for j in range(4) for i in range(j, 4)]

    def multiply(i, j, step):
        start, count = LOADS[step]
        cols = slice(start, start + count)
        left = wt[2 * i : 2 * i + 2, :, cols].reshape(2 * LANES, count)
        if i == j:
            left = jnp.concatenate([left, row_obs[:, cols]], axis=0)
        right = wt[2 * j : 2 * j + 2, :, cols].reshape(2 * LANES, count)
        product = lax.dot_general(left, right, NT, preferred_element_type=F32)
        place, lines = squares.index((i, j)), product.shape[0]
        if step:
            product = product + partial[place, :lines]
        if step + 1 < CHUNKS:
            partial[place, :lines] = product
        else:
            keep(i, j, product)

    def keep(i, j, product):
        for a in range(2):
            for b in range(2):
                value = product[a * LANES : (a + 1) * LANES, b * LANES : (b + 1) * LANES]
                store(2 * i + a, 2 * j + b, value)
                if i > j:
                    store(2 * j + b, 2 * i + a, value.T)
        if i == j:
            line = 2 * LANES
            rhs = product[line : line + 1] + product[line + 1 : line + 2]
            for b in range(2):
                high, core = block_at(2 * j + b)
                extra_core[c, pl.ds(2 * high + core, 1), :] = rhs[:, b * LANES : (b + 1) * LANES]

    def panel(k, step=CHUNKS - 1):
        for i in range(k, 4):
            multiply(i, k, step)

    exchanged = {}

    def exchange(j):
        pairs = [(j, i) for i in range(j, 4)] + [(i, j) for i in range(j + 1, 4)]
        for k, i in pairs:
            line = (y + OFFSETS[i]) % 4
            exchanged[k, i] = send(other.at[k, line], arrived.at[k, line], partner)

    def merge(k):
        for i in range(4):
            exchanged[k, i].wait_recv()

        def add(i, _):
            own[k, i] = own[k, i] + arrived[k, i]
            return 0

        lax.fori_loop(0, 4, add, 0)

    def scatter(axis, src, bufs):
        to = axis_device[axis]
        return [(prepare(src(d), bufs.at[d - 1], to(d)), bufs.at[d - 1]) for d in (2, 1, 3)]

    def start(copies):
        for copy, _ in copies:
            copy.start()
        return copies

    def gather(src, copies):
        for copy, _ in copies:
            copy.wait_recv()
        mine = src(0)
        total = mine[...]
        for _, buf in copies:
            total = total + buf[...]
        mine[...] = total

    class Ring:
        def __init__(self, axis, src, bufs):
            right, left = axis_device[axis](1), axis_device[axis](3)
            self.src, self.bufs = src, bufs
            self.hop_a = prepare(src(2, 0), bufs.at[0], right)
            self.hop_b = prepare(src(2, 1), bufs.at[1], left)
            self.direct_b = prepare(src(1, 1), bufs.at[3], right)
            self.direct_a = prepare(src(3, 0), bufs.at[2], left)
            self.last_a = prepare(bufs.at[0], bufs.at[4], right)
            self.last_b = prepare(bufs.at[1], bufs.at[5], left)
            self.next_a, self.next_b = src(1, 0), src(3, 1)

        def start_far(self):
            self.hop_a.start()
            self.hop_b.start()

        def start_right(self):
            self.direct_b.start()

        def start_left(self):
            self.direct_a.start()

        def start(self):
            self.start_far()
            self.start_right()
            self.start_left()

        def pass_right(self):
            self.hop_a.wait_recv()
            self.bufs[0] = self.bufs[0] + self.next_a[...]
            self.last_a.start()

        def pass_left(self):
            self.hop_b.wait_recv()
            self.bufs[1] = self.bufs[1] + self.next_b[...]
            self.last_b.start()

        def finish(self):
            for half, direct, via in ((0, self.direct_a, self.last_a), (1, self.direct_b, self.last_b)):
                direct.wait_recv()
                via.wait_recv()
                mine = self.src(0, half)
                mine[...] = mine[...] + self.bufs[2 + half] + self.bufs[4 + half]

    panel_of = {2: 0, 1: 1, 3: 2, 0: 3}

    def at(part, k, dz, dx):
        return own.at[k, dz, dx, part_rows(part), :]

    every = slice(None)

    def two(half):
        return pl.ds(2 * half, 2)

    def half_x(k):
        return lambda d, half: at(0, k, two(half), (x + d) % 4)

    def half_z(k):
        return lambda d, half: at(2, k, (z + d) % 4, two(half))

    def half_y(d, half):
        return at(1, panel_of[d], two(half), every)

    def src_x(k):
        return lambda d: at(0, k, every, (x + d) % 4)

    def src_z(k):
        return lambda d: at(2, k, (z + d) % 4, every)

    def src_0y(d):
        return at(0, panel_of[d], every, x)

    def src_1z(d):
        return at(1, 3, (z + d) % 4, every)

    def src_2x(k):
        return lambda d: at(2, k, z, (x + d) % 4)

    def src_0z(d):
        return at(0, 3, (z + d) % 4, x)

    def src_1x(d):
        return at(1, 3, z, (x + d) % 4)

    def src_2y(d):
        return at(2, panel_of[d], z, x)

    to_y = axis_device["y"]
    distance_of = (2, 1, 3, 0)
    step_0y, step_2x, step_2y = [], {}, []
    rings = {k: (Ring("x", half_x(k), ring_x.at[k]), Ring("z", half_z(k), ring_z.at[k])) for k in range(RINGS)}
    ring_of_y = Ring("y", half_y, ring_y)

    step_x = {k: scatter("x", src_x(k), first_x.at[k - RINGS]) for k in range(RINGS, 4)}
    step_z = {k: scatter("z", src_z(k), first_z.at[k - RINGS]) for k in range(RINGS, 4)}

    def spread(k):
        if k < RINGS:
            for ring in rings[k]:
                ring.start()
        else:
            start(step_x[k])
            start(step_z[k])
        if k == 0:
            ring_of_y.start_far()
        if k == 1:
            ring_of_y.start_right()
        if k == 2:
            ring_of_y.start_left()

    def pass_on(k):
        for ring in rings[k]:
            ring.pass_right()
            ring.pass_left()

    def finish_x(k):
        if k < RINGS:
            rings[k][0].finish()
        else:
            gather(src_x(k), step_x[k])

    def finish_z(k):
        if k < RINGS:
            rings[k][1].finish()
        else:
            gather(src_z(k), step_z[k])

    def gather_extra(stage, copies):
        for copy in copies:
            copy.wait_recv()
        total = extra_ring[stage, 0] + extra_ring[stage, 1]
        return total + extra_ring[stage, 2] + extra_ring[stage, 3]

    def spread_extra(stage, total):
        place = (x, y, z)[stage]
        to = axis_device["xyz"[stage]]
        extra_ring[stage, place] = total
        slot = extra_ring.at[stage, place]
        return [send(slot, slot, to(d)) for d in (2, 1, 3)]

    weigh(0)
    for step in range(1, CHUNKS):
        weigh(step)
        for k in range(4):
            panel(k, step - 1)
    panel(0)
    pl.semaphore_wait(barrier, len(peers))
    exchange(0)
    panel(1)
    exchange(1)
    panel(2)
    exchange(2)
    panel(3)
    slot = extra_core.at[c]
    sent_extra = send(slot, slot, partner)
    exchange(3)
    merge(0)
    spread(0)
    merge(1)
    spread(1)
    merge(2)
    spread(2)
    sent_extra.wait_recv()
    extra = spread_extra(0, extra_core[0] + extra_core[1])
    pass_on(0)
    merge(3)
    spread(3)
    ring_of_y.pass_right()
    ring_of_y.pass_left()
    for k in range(1, RINGS):
        pass_on(k)
    def finish(k):
        finish_x(k)
        if k < 3:
            d = distance_of[k]
            step_0y.append((send(src_0y(d), second_0.at[k], to_y(d)), second_0.at[k]))
        finish_z(k)
        step_2x[k] = start(scatter("x", src_2x(k), second_2.at[k]))

    extra = spread_extra(1, gather_extra(0, extra))
    finish(0)
    finish(1)
    ring_of_y.finish()
    step_1z = start(scatter("z", src_1z, second_1))
    extra = spread_extra(2, gather_extra(1, extra))
    finish(2)
    finish(3)
    gather(src_0y, step_0y)
    step_0z = start(scatter("z", src_0z, last_0))
    for k in range(4):
        gather(src_2x(k), step_2x[k])
        if k < 3:
            d = distance_of[k]
            step_2y.append((send(src_2y(d), last_2.at[k], to_y(d)), last_2.at[k]))
    gather(src_1z, step_1z)
    step_1x = start(scatter("x", src_1x, last_1))
    for part, src, copies in ((0, src_0z, step_0z), (2, src_2y, step_2y), (1, src_1x, step_1x)):
        for copy, _ in copies:
            copy.wait_recv()
        total = src(0)[...]
        for _, buf in copies:
            total = total + buf[...]
        out[part_rows(part), :] = total * (1.0 / TOTAL)
    out_extra[...] = gather_extra(2, extra) * (1.0 / TOTAL)
    for copy in started:
        copy.wait_send()


def split(gram, extra, out_gram, out_rhs, out_chi):
    r, g = lax.axis_index("rows"), lax.axis_index("grid")
    out_gram[...] = gram[...]
    line = extra[pl.ds(r // 2, 1), :]
    line = pltpu.roll(line, (2 * LANES - (64 * (r % 2) + 8 * g)) % LANES, 1)
    out_rhs[...] = line[0, :8]
    out_chi[0] = extra[BLOCKS, 0]


COPIES = 16 + 2 * (6 * RINGS + 3 * (4 - RINGS)) + 6 + 3 + 3 + 12 + 9 + 10


def local(design, observed, weight_class, calib_unit, class_weight, calib_scale):
    dense = (ROWS // LANES, LANES)
    vmem = pl.BlockSpec(memory_space=pltpu.VMEM)
    panels = pltpu.VMEM((4, 4, 4, TILE, LANES), F32)
    rows_x, rows_y, rows_z = (rows for _, rows in PARTS)
    gram, extra = pl.pallas_call(
        kernel,
        out_shape=(jax.ShapeDtypeStruct((TILE, LANES), F32), jax.ShapeDtypeStruct((EXTRA, LANES), F32)),
        in_specs=[pl.BlockSpec(memory_space=pltpu.HBM)] * 6,
        out_specs=(vmem, vmem),
        scratch_shapes=[
            pltpu.VMEM((ROWS, WIDTH), BF16),
            pltpu.VMEM((BLOCKS, LANES, ROWS), BF16),
            pltpu.VMEM((BLOCKS, ROWS), F32),
            pltpu.VMEM((EXTRA, ROWS), BF16),
            panels, panels, panels,
            pltpu.VMEM((10, 2 * LANES + EXTRA, 2 * LANES), F32),
            pltpu.VMEM((RINGS, 6, 2, rows_x, LANES), F32),
            pltpu.VMEM((RINGS, 6, 2, rows_z, LANES), F32),
            pltpu.VMEM((6, 2, 4, rows_y, LANES), F32),
            pltpu.VMEM((4 - RINGS, 3, 4, rows_x, LANES), F32),
            pltpu.VMEM((4 - RINGS, 3, 4, rows_z, LANES), F32),
            pltpu.VMEM((3, 4, rows_x, LANES), F32),
            pltpu.VMEM((3, 4, rows_y, LANES), F32),
            pltpu.VMEM((4, 3, rows_z, LANES), F32),
            pltpu.VMEM((3, rows_x, LANES), F32),
            pltpu.VMEM((3, rows_y, LANES), F32),
            pltpu.VMEM((3, rows_z, LANES), F32),
            pltpu.VMEM((2, EXTRA, LANES), F32),
            pltpu.VMEM((3, 4, EXTRA, LANES), F32),
            pltpu.VMEM(dense, F32),
            pltpu.VMEM(dense, jnp.int32),
            pltpu.VMEM(dense, jnp.int32),
            pltpu.SMEM((CLASSES,), F32),
            pltpu.VMEM((BLOCKS, UNITS), F32),
            pltpu.SemaphoreType.DMA((CHUNKS,)),
            pltpu.SemaphoreType.DMA((5,)),
            pltpu.SemaphoreType.DMA((COPIES,)),
            pltpu.SemaphoreType.DMA((COPIES,)),
        ],
        compiler_params=pltpu.CompilerParams(
            collective_id=0, has_side_effects=True, vmem_limit_bytes=32 * 2**20
        ),
    )(
        *[pltpu.with_memory_space_constraint(v, pltpu.HBM) for v in (design,
        observed.reshape(dense),
        weight_class.reshape(dense),
        calib_unit.reshape(dense),
        class_weight,
        calib_scale.T)],
    )
    gram, right_hand, chi = pl.pallas_call(
        split,
        out_shape=(
            jax.ShapeDtypeStruct((TILE, LANES), F32),
            jax.ShapeDtypeStruct((8,), F32),
            jax.ShapeDtypeStruct((1,), F32),
        ),
        in_specs=[vmem, vmem],
        out_specs=(vmem, vmem, pl.BlockSpec(memory_space=pltpu.SMEM)),
        compiler_params=pltpu.CompilerParams(vmem_limit_bytes=2**20),
    )(gram, extra)
    return gram, right_hand, chi.reshape(())


def solution(mesh):
    both = ("rows", "grid")
    return jax.shard_map(
        local,
        mesh=mesh,
        in_specs=(P(both, None), P(both), P(both), P(both), P(), P()),
        out_specs=(P("rows", "grid"), P(both), P()),
        check_vma=False,
    )
```
